32 devices in a mesh: lev: 4 (over z), wav: 8 (over y, x, core).
Axes of the slice: x: 2, y: 2, z: 4, core: 2. Of those that a mesh axis runs over, the one named last changes fastest.
Arguments:
- grid_field: float32 [8, 1216, 1216], P('lev', 'wav'), may hold values from -6 to 6
- truncation_limit: int32 [1216], replicated, may hold values from -1 to 607, as said below
- diffusion_order: int32 [8], P('lev'), may hold values from 1 to 4
- diffusion_strength: float32 [8], P('lev'), may hold values from 2 to 50
- mass_weight: float32 [8], P('lev'), may hold values from 0.25 to 4
Outputs:
- filtered: float32 [8, 1216, 1216], P('lev', 'wav')
- energies: float32 [8], P('lev')
- total_energy: float32 [], replicated
The draws below stay inside these ranges and needn't reach their ends.
Inputs may be any that keep to these rules, and one draw needn't show every extreme that they name: `truncation_limit`: the largest |wavenumber(q)| kept at index p, with wavenumber(m) = m below 608 and m - 1216 otherwise; the kept set is an ellipse about wavenumber zero; the value at p equals the value at 1216 - p; -1 where nothing is kept; the value at p = 0 is 607.
All inputs are finite; a program needn't handle non-finite values.
Results may differ from the reference program's by a relative error of at most 0.000071.
Values sent between devices are 32-bit elements.
A program may use at most 64 MiB of HBM per device.

```python
import math
import jax
import jax.numpy as jnp
from jax import lax

N = 1216
SLABS = 8


def draw_truncation_limit(key, part):
    axis_second = jax.random.randint(key, (), 3 * N // 10, N // 2)
    axis_first = N // 2 - 1
    positions = jnp.arange(N, dtype=jnp.int32)
    distance = jnp.abs(jnp.where(positions < N // 2, positions, positions - N))
    steps_first = jnp.arange(N // 2 + 1, dtype=jnp.int32)
    scaled_second = distance * 1000 // axis_second
    scaled_first = steps_first * 1000 // axis_first
    inside = scaled_second[:, None] ** 2 + scaled_first[None, :] ** 2 <= 1000000
    return (jnp.sum(inside.astype(jnp.int32), axis=1) - 1).astype(jnp.int32)


def set_ends(drawn, key, smallest, largest):
    place = [jax.random.randint(jax.random.fold_in(key, axis), (), 0, length) for axis, length in enumerate(drawn.shape)]
    longest = drawn.shape.index(max(drawn.shape))
    neighbour = place[:longest] + [(place[longest] + 1) % drawn.shape[longest]] + place[longest + 1:]
    return drawn.at[tuple(place)].set(smallest).at[tuple(neighbour)].set(largest)


def block_levels(key, extent, pieces, low, largest):
    loudness, own = 1.0, jax.random.fold_in(key, 6)
    for position, shards_of in pieces:
        draws = jnp.exp(jax.random.uniform(jax.random.fold_in(own, position), (shards_of,), jnp.float32, low / len(pieces), largest / len(pieces)))
        loudness = loudness * jnp.repeat(draws, extent[position] // shards_of).reshape([-1 if axis == position else 1 for axis in range(len(extent))])
    return loudness


def centred(own_key, extent, spread, bound, split=(), kind=jnp.bfloat16):
    gain = block_levels(own_key, extent, split, -0.22, 0.18) if split else 1.0
    drawn = jax.random.normal(own_key, extent, jnp.float32) * spread * gain
    return jnp.minimum(jnp.maximum(drawn, -bound), bound).astype(kind)


def setup_inputs(seed: int = 0) -> dict:
    key_list = jax.random.split(jax.random.key(seed), 6)
    grid_field = centred(key_list[0], (SLABS, N, N), 1.0, 6.0, ((0, 4), (1, 8)), jnp.float32)
    truncation_limit = draw_truncation_limit(jax.random.fold_in(key_list[5], 71), 0)
    diffusion_order = set_ends(jax.random.randint(key_list[2], (SLABS,), 1, 5), jax.random.fold_in(key_list[2], 1), 1, 4).astype(jnp.int32)
    diffusion_strength = jnp.clip(jnp.exp(math.log(50.0) - 3.218876 * jax.random.uniform(key_list[3], (SLABS,), jnp.float32) ** block_levels(key_list[3], (SLABS,), ((0, 4),), -0.2, 0.2)), 2.0, 50.0)
    mass_weight = jnp.clip(jnp.exp(math.log(4.0) - 2.7725887 * jax.random.uniform(key_list[4], (SLABS,), jnp.float32) ** block_levels(key_list[4], (SLABS,), ((0, 4),), -0.2, 0.2)), 0.25, 4.0)
    return dict(grid_field=grid_field, truncation_limit=truncation_limit, diffusion_order=diffusion_order, diffusion_strength=diffusion_strength, mass_weight=mass_weight)


def signed(positions, length):
    return jnp.where(positions < length // 2, positions, positions - length)


def reference(grid_field, truncation_limit, diffusion_order, diffusion_strength, mass_weight):
    positions = jnp.arange(N, dtype=jnp.int32)
    signed_index = signed(positions, N)
    wavenumber = signed_index.astype(jnp.float32)
    scaled_radius = (wavenumber[:, None] ** 2 + wavenumber[None, :] ** 2) / (0.5 * N) ** 2
    inside = (jnp.abs(signed_index)[None, :] <= truncation_limit[:, None]).astype(jnp.float32)

    def one_slab(members):
        slab_field, degree, strength = members
        spectrum = jnp.fft.fft2(slab_field).T
        damping = inside / (1.0 + strength * jnp.power(scaled_radius, degree.astype(jnp.float32)))
        damped = spectrum * damping
        energy = jnp.sum(jnp.real(damped) ** 2 + jnp.imag(damped) ** 2) / float(N) ** 4
        filtered = jnp.real(jnp.fft.ifft2(damped.T))
        return filtered, energy

    filtered, energies = lax.map(one_slab, (grid_field, diffusion_order, diffusion_strength))
    total_energy = jnp.sum(mass_weight * energies) / SLABS
    return filtered, energies, total_energy
```

```python
import jax
import jax.numpy as jnp
import numpy as np
from jax import lax
from jax.sharding import PartitionSpec as P

product_precision = lax.Precision.HIGH


def tables(length):
    step = 32
    coarse = -(-length // step)
    columns = np.arange(length)
    high = 2.0 * np.pi / length * (np.arange(coarse)[:, None] * step * columns[None, :] % length)
    low = 2.0 * np.pi / length * (np.arange(step)[:, None] * columns[None, :] % length)
    cos_high, sin_high = (jnp.asarray(f(high), jnp.float32)[:, None] for f in (np.cos, np.sin))
    cos_low, sin_low = (jnp.asarray(f(low), jnp.float32)[None] for f in (np.cos, np.sin))
    cosine = cos_high * cos_low - sin_high * sin_low
    sine = sin_high * cos_low + cos_high * sin_low
    return tuple(t.reshape(coarse * step, length)[:length] for t in (cosine, sine))


def signed(positions, length):
    return jnp.where(positions < length // 2, positions, positions - length)


def transform(values, cosine_table, sine_table, direction):
    with_cosine = jnp.einsum("scpi,iq->scpq", values, cosine_table, precision=product_precision)
    with_sine = jnp.einsum("scpi,iq->scpq", values, sine_table, precision=product_precision)
    if direction < 0:
        real_part = with_cosine[:, 0] + with_sine[:, 1]
        imaginary = with_cosine[:, 1] - with_sine[:, 0]
    else:
        real_part = with_cosine[:, 0] - with_sine[:, 1]
        imaginary = with_cosine[:, 1] + with_sine[:, 0]
    return jnp.stack([real_part, imaginary], axis=1)


def damping(wave_rows, limits, length, diffusion_order, diffusion_strength):
    wave_first = signed(jnp.arange(length, dtype=jnp.int32), length)
    rows_float = wave_rows.astype(jnp.float32)
    first_float = wave_first.astype(jnp.float32)
    scaled_radius = (rows_float[:, None] ** 2 + first_float[None, :] ** 2) / (0.5 * length) ** 2
    inside = (jnp.abs(wave_first)[None, :] <= limits[:, None]).astype(jnp.float32)
    powered = jnp.power(scaled_radius[None], diffusion_order.astype(jnp.float32)[:, None, None])
    return inside[None] / (1.0 + diffusion_strength[:, None, None] * powered)


def mirrored(values):
    return jnp.roll(jnp.flip(values, -1), 1, -1)


def half_plane(
    grid_field, truncation_limit, diffusion_order, diffusion_strength, cosine_table, sine_table
):
    length = grid_field.shape[2]
    half = length // 2
    row_real = jnp.einsum("sij,jl->sli", grid_field, cosine_table[:, :half], precision=product_precision)
    row_imag = -jnp.einsum("sij,jl->sli", grid_field, sine_table[:, :half], precision=product_precision)
    nyquist = jnp.einsum("sij,j->si", grid_field, cosine_table[:, half], precision=product_precision)
    zero_row = (jnp.arange(half, dtype=jnp.int32) == 0)[None, :, None]
    row_imag = jnp.where(zero_row, nyquist[:, None, :], row_imag)
    along_rows = jnp.stack([row_real, row_imag], axis=1)
    spectrum = transform(
        lax.all_to_all(along_rows, "wav", split_axis=2, concat_axis=3, tiled=True),
        cosine_table,
        sine_table,
        -1,
    )
    column_count = spectrum.shape[2]
    wav_index = lax.axis_index("wav")
    offset = wav_index * column_count
    wave_rows = offset + jnp.arange(column_count, dtype=jnp.int32)
    limits = lax.dynamic_slice(truncation_limit, (offset,), (column_count,))
    damp_main = damping(wave_rows, limits, length, diffusion_order, diffusion_strength)
    nyquist_rows = signed(jnp.full((1,), half, jnp.int32), length)
    damp_top = damping(
        nyquist_rows, truncation_limit[half : half + 1], length, diffusion_order, diffusion_strength
    )[:, 0]
    damped = spectrum * damp_main[:, None]
    packed_real = spectrum[:, 0, 0, :]
    packed_imag = spectrum[:, 1, 0, :]
    back_real = mirrored(packed_real)
    back_imag = mirrored(packed_imag)
    zero_real = (packed_real + back_real) * 0.5 * damp_main[:, 0]
    zero_imag = (packed_imag - back_imag) * 0.5 * damp_main[:, 0]
    top_real = (packed_imag + back_imag) * 0.5 * damp_top
    top_imag = (back_real - packed_real) * 0.5 * damp_top
    is_zero = wave_rows == 0
    column_weight = jnp.where(is_zero, 0.0, 2.0).astype(jnp.float32)
    edge = jnp.sum(zero_real**2 + zero_imag**2 + top_real**2 + top_imag**2, axis=-1)
    main_sum = jnp.sum(damped * damped * column_weight[None, None, :, None], axis=(1, 2, 3))
    partial_value = (main_sum + jnp.where(wav_index == 0, edge, 0.0)) / float(length) ** 4
    zero_column = is_zero[None, :, None]
    repacked = jnp.stack(
        [
            jnp.where(zero_column, (zero_real - top_imag)[:, None, :], damped[:, 0]),
            jnp.where(zero_column, (zero_imag + top_real)[:, None, :], damped[:, 1]),
        ],
        axis=1,
    )
    along_first = transform(repacked, cosine_table, sine_table, 1)
    inverse_area = 1.0 / float(length) ** 2
    received = lax.all_to_all(along_first, "wav", split_axis=3, concat_axis=2, tiled=True)
    row_weight = jnp.where(jnp.arange(half, dtype=jnp.int32) == 0, 1.0, 2.0).astype(jnp.float32)[
        :, None
    ]
    with_cosine = jnp.einsum(
        "spi,pj->sij", received[:, 0] * row_weight, cosine_table[:half], precision=product_precision
    )
    with_sine = jnp.einsum(
        "spi,pj->sij", received[:, 1] * row_weight, sine_table[:half], precision=product_precision
    )
    top_term = received[:, 1, 0, :][:, :, None] * cosine_table[half][None, None, :]
    filtered = (with_cosine - with_sine + top_term) * inverse_area
    return (filtered, partial_value)


def local(grid_field, truncation_limit, diffusion_order, diffusion_strength, mass_weight):
    slab_count, row_count, length = grid_field.shape
    cosine_table, sine_table = tables(length)
    filtered, partial_value = half_plane(
        grid_field, truncation_limit, diffusion_order, diffusion_strength, cosine_table, sine_table
    )
    total_slabs = lax.axis_size("lev") * slab_count
    energies = lax.psum(partial_value, "wav")
    weighted_sum = lax.psum(jnp.sum(mass_weight * energies), "lev")
    total_energy = weighted_sum / total_slabs
    return (filtered, energies, total_energy)


def solution(mesh):
    placed = (P("lev", "wav", None), P(), P("lev"), P("lev"), P("lev"))
    return jax.shard_map(
        local,
        mesh=mesh,
        in_specs=placed,
        out_specs=(P("lev", "wav", None), P("lev"), P()),
        check_vma=False,
    )
```

```python
import functools

import jax
import jax.numpy as jnp
import numpy as np
from jax import lax
from jax.experimental import pallas as pl
from jax.experimental.pallas import tpu as pltpu
from jax.sharding import PartitionSpec as P

product_precision = lax.Precision.HIGH


def tables(length):
    step = 32
    coarse = -(-length // step)
    columns = np.arange(length)
    high = 2.0 * np.pi / length * (np.arange(coarse)[:, None] * step * columns[None, :] % length)
    low = 2.0 * np.pi / length * (np.arange(step)[:, None] * columns[None, :] % length)
    cos_high, sin_high = (jnp.asarray(f(high), jnp.float32)[:, None] for f in (np.cos, np.sin))
    cos_low, sin_low = (jnp.asarray(f(low), jnp.float32)[None] for f in (np.cos, np.sin))
    cosine = cos_high * cos_low - sin_high * sin_low
    sine = sin_high * cos_low + cos_high * sin_low
    return tuple(t.reshape(coarse * step, length)[:length] for t in (cosine, sine))


def signed(positions, length):
    return jnp.where(positions < length // 2, positions, positions - length)


def transform(values, cosine_table, sine_table, direction):
    with_cosine = jnp.einsum("scpi,iq->scpq", values, cosine_table, precision=product_precision)
    with_sine = jnp.einsum("scpi,iq->scpq", values, sine_table, precision=product_precision)
    if direction < 0:
        real_part = with_cosine[:, 0] + with_sine[:, 1]
        imaginary = with_cosine[:, 1] - with_sine[:, 0]
    else:
        real_part = with_cosine[:, 0] - with_sine[:, 1]
        imaginary = with_cosine[:, 1] + with_sine[:, 0]
    return jnp.stack([real_part, imaginary], axis=1)


def damping(wave_rows, limits, length, diffusion_order, diffusion_strength):
    wave_first = signed(jnp.arange(length, dtype=jnp.int32), length)
    rows_float = wave_rows.astype(jnp.float32)
    first_float = wave_first.astype(jnp.float32)
    scaled_radius = (rows_float[:, None] ** 2 + first_float[None, :] ** 2) / (0.5 * length) ** 2
    inside = (jnp.abs(wave_first)[None, :] <= limits[:, None]).astype(jnp.float32)
    powered = jnp.power(scaled_radius[None], diffusion_order.astype(jnp.float32)[:, None, None])
    return inside[None] / (1.0 + diffusion_strength[:, None, None] * powered)


def mirrored(values):
    return jnp.roll(jnp.flip(values, -1), 1, -1)


def half_plane(
    grid_field, truncation_limit, diffusion_order, diffusion_strength, cosine_table, sine_table
):
    length = grid_field.shape[2]
    half = length // 2
    row_real = jnp.einsum("sij,jl->sli", grid_field, cosine_table[:, :half], precision=product_precision)
    row_imag = -jnp.einsum("sij,jl->sli", grid_field, sine_table[:, :half], precision=product_precision)
    nyquist = jnp.einsum("sij,j->si", grid_field, cosine_table[:, half], precision=product_precision)
    zero_row = (jnp.arange(half, dtype=jnp.int32) == 0)[None, :, None]
    row_imag = jnp.where(zero_row, nyquist[:, None, :], row_imag)
    along_rows = jnp.stack([row_real, row_imag], axis=1)
    spectrum = transform(
        lax.all_to_all(along_rows, "wav", split_axis=2, concat_axis=3, tiled=True),
        cosine_table,
        sine_table,
        -1,
    )
    column_count = spectrum.shape[2]
    wav_index = lax.axis_index("wav")
    offset = wav_index * column_count
    wave_rows = offset + jnp.arange(column_count, dtype=jnp.int32)
    limits = lax.dynamic_slice(truncation_limit, (offset,), (column_count,))
    damp_main = damping(wave_rows, limits, length, diffusion_order, diffusion_strength)
    nyquist_rows = signed(jnp.full((1,), half, jnp.int32), length)
    damp_top = damping(
        nyquist_rows, truncation_limit[half : half + 1], length, diffusion_order, diffusion_strength
    )[:, 0]
    damped = spectrum * damp_main[:, None]
    packed_real = spectrum[:, 0, 0, :]
    packed_imag = spectrum[:, 1, 0, :]
    back_real = mirrored(packed_real)
    back_imag = mirrored(packed_imag)
    zero_real = (packed_real + back_real) * 0.5 * damp_main[:, 0]
    zero_imag = (packed_imag - back_imag) * 0.5 * damp_main[:, 0]
    top_real = (packed_imag + back_imag) * 0.5 * damp_top
    top_imag = (back_real - packed_real) * 0.5 * damp_top
    is_zero = wave_rows == 0
    column_weight = jnp.where(is_zero, 0.0, 2.0).astype(jnp.float32)
    edge = jnp.sum(zero_real**2 + zero_imag**2 + top_real**2 + top_imag**2, axis=-1)
    main_sum = jnp.sum(damped * damped * column_weight[None, None, :, None], axis=(1, 2, 3))
    partial_value = (main_sum + jnp.where(wav_index == 0, edge, 0.0)) / float(length) ** 4
    zero_column = is_zero[None, :, None]
    repacked = jnp.stack(
        [
            jnp.where(zero_column, (zero_real - top_imag)[:, None, :], damped[:, 0]),
            jnp.where(zero_column, (zero_imag + top_real)[:, None, :], damped[:, 1]),
        ],
        axis=1,
    )
    along_first = transform(repacked, cosine_table, sine_table, 1)
    inverse_area = 1.0 / float(length) ** 2
    received = lax.all_to_all(along_first, "wav", split_axis=3, concat_axis=2, tiled=True)
    row_weight = jnp.where(jnp.arange(half, dtype=jnp.int32) == 0, 1.0, 2.0).astype(jnp.float32)[
        :, None
    ]
    with_cosine = jnp.einsum(
        "spi,pj->sij", received[:, 0] * row_weight, cosine_table[:half], precision=product_precision
    )
    with_sine = jnp.einsum(
        "spi,pj->sij", received[:, 1] * row_weight, sine_table[:half], precision=product_precision
    )
    top_term = received[:, 1, 0, :][:, :, None] * cosine_table[half][None, None, :]
    filtered = (with_cosine - with_sine + top_term) * inverse_area
    return (filtered, partial_value)


LANES = 128
MESH = pl.DeviceIdType.MESH


def halves(values):
    high = values.astype(jnp.bfloat16)
    return high, (values - high.astype(jnp.float32)).astype(jnp.bfloat16)


def product(left, right):
    dot = functools.partial(jnp.dot, preferred_element_type=jnp.float32)
    return dot(left[0], right[0]) + dot(left[1], right[0]) + dot(left[0], right[1])


def times_i(value, sign):
    return (-value[1], value[0]) if sign > 0 else (value[1], -value[0])


def plus(a, b):
    return (a[0] + b[0], a[1] + b[1])


def minus(a, b):
    return (a[0] - b[0], a[1] - b[1])


def eight_points(x, sign):
    def four(p, q, r, t):
        a0, a1, a2, a3 = plus(p, r), minus(p, r), plus(q, t), times_i(minus(q, t), sign)
        return plus(a0, a2), plus(a1, a3), minus(a0, a2), minus(a1, a3)

    e = four(x[0], x[2], x[4], x[6])
    o = four(x[1], x[3], x[5], x[7])
    root = 0.5**0.5
    o2 = times_i(o[2], sign)
    i1, i3 = times_i(o[1], sign), times_i(o[3], sign)
    o1 = tuple(root * v for v in plus(o[1], i1))
    o3 = tuple(root * v for v in minus(i3, o[3]))
    odd = (o[0], o1, o2, o3)
    return [plus(e[n], odd[n]) for n in range(4)] + [minus(e[n], odd[n]) for n in range(4)]


def pieces(rows, group_rows, groups):
    found = []
    for group in range(groups):
        start, stop = group * group_rows, min((group + 1) * group_rows, 2 * rows)
        while start < stop:
            part = start // rows
            end = min(stop, (part + 1) * rows)
            found.append((group, start - group * group_rows, part, start - part * rows, end - start))
            start = end
    return found


def fused_kernel(
    sizes,
    grid_ref, limit_ref, order_ref, strength_ref, mass_ref, coarse_ref, fine_ref,
    back_coarse_hbm, back_fine_hbm, twiddle_hbm, base_hbm,
    out_ref, energy_ref, total_ref,
    grid_parts, table, back_table, back_coarse, back_fine, twiddle, base,
    sent, got, sent_back, got_back, rest, work, damp, energy_mine, energy_all,
    load_sems, send_sems, recv_sems, back_send_sems, back_recv_sems, e_send_sems, e_recv_sems, local_sems,
):
    slabs, rows, length, wav, lev, quarters, columns, padded, tail, groups, group_rows = sizes
    everyone = lev * wav
    half = length // 2
    wide = 2 * LANES
    me = lax.axis_index("wav")
    level = lax.axis_index("lev")
    my_quarter, my_slab = me // slabs, me % slabs
    flat = level * wav + me

    def other(step):
        target = (flat + step) % everyone
        return target // wav, target % wav

    barrier = pltpu.get_barrier_semaphore()

    @pl.loop(1, everyone)
    def _(step):
        pl.semaphore_signal(barrier, inc=1, device_id=other(step), device_id_type=MESH)

    loads = [
        pltpu.make_async_copy(src, dst, load_sems.at[n])
        for n, (src, dst) in enumerate(
            ((back_coarse_hbm, back_coarse), (back_fine_hbm, back_fine), (twiddle_hbm, twiddle), (base_hbm, base))
        )
    ]
    for load in loads:
        load.start()
    high, low = halves(grid_ref[...])
    grid_parts[0] = high
    grid_parts[1] = low

    def quarter_of(step):
        down, across = 1 - step % 2, 1 - step // 2
        y, x = my_quarter // 2, my_quarter % 2
        return (y + down - 2 * y * down) * 2 + (x + across - 2 * x * across)

    def remote(source, target, send, recv, w):
        return pltpu.make_async_remote_copy(
            src_ref=source.at[w], dst_ref=target.at[me], send_sem=send.at[w], recv_sem=recv.at[me],
            device_id=(level, w), device_id_type=MESH,
        )

    def push(source, target, send, recv, w, local_sem):
        @pl.when(w != me)
        def _():
            remote(source, target, send, recv, w).start()

        @pl.when(w == me)
        def _():
            pltpu.make_async_copy(source.at[w], target.at[w], local_sem).start()

    def arrive(source, target, send, recv, w, local_sem):
        @pl.when(w != me)
        def _():
            pltpu.make_async_remote_copy(
                src_ref=source.at[w], dst_ref=target.at[w], send_sem=send.at[w], recv_sem=recv.at[w],
                device_id=(level, w), device_id_type=MESH,
            ).wait()

        @pl.when(w == me)
        def _():
            pltpu.make_async_copy(source.at[w], target.at[w], local_sem).wait()

    lane = lax.broadcasted_iota(jnp.int32, (1, LANES), 1)
    layout = pieces(rows, group_rows, groups)

    @pl.loop(0, quarters)
    def _(step):
        quarter = quarter_of(step)

        @pl.loop(0, length // 16)
        def _(block):
            cos_c, sin_c = coarse_ref[0, quarter, pl.ds(block, 1)], coarse_ref[1, quarter, pl.ds(block, 1)]
            cos_f, sin_f = fine_ref[0, quarter], fine_ref[1, quarter]
            span = pl.ds(pl.multiple_of(block * 16, 16), 16)
            for part, value in enumerate((cos_c * cos_f - sin_c * sin_f, -(sin_c * cos_f + cos_c * sin_f))):
                value_high, value_low = halves(value)
                table[0, span, part * wide : (part + 1) * wide] = value_high
                table[1, span, part * wide : (part + 1) * wide] = value_low

        result = product((grid_parts[0], grid_parts[1]), (table[0], table[1]))
        for slab in range(slabs):
            w = quarter * slabs + slab
            block = result[slab * rows : (slab + 1) * rows]
            for part in range(2):
                sent[w, part * rows : (part + 1) * rows] = block[:, part * wide : part * wide + LANES]
            packed = jnp.zeros((group_rows, LANES), jnp.float32)
            shifted = {}
            for group, at, part, start, count in layout:
                piece = block[start : start + count, part * wide + LANES : (part + 1) * wide]
                piece = jnp.where(lane < tail, piece, 0.0)
                shifted.setdefault(group, []).append(pltpu.roll(piece, group * tail, 1) if group else piece)
            for group, found in shifted.items():
                whole = jnp.concatenate(found, 0) if len(found) > 1 else found[0]
                if whole.shape[0] < group_rows:
                    fill = jnp.zeros((group_rows - whole.shape[0], LANES), jnp.float32)
                    whole = jnp.concatenate([whole, fill], 0)
                packed = packed + whole
            sent[w, 2 * rows :] = packed

        @pl.when(step == 0)
        def _():
            pl.semaphore_wait(barrier, everyone - 1)

        for slab in range(slabs):
            push(sent, got, send_sems, recv_sems, quarter * slabs + slab, local_sems.at[0])

    for load in loads:
        load.wait()

    wide_lane = lax.broadcasted_iota(jnp.int32, (1, wide), 1)
    wave = my_quarter * columns + wide_lane
    valid = (wide_lane < columns) | ((wide_lane == columns) & (wave == half))
    single = (wave == 0) | (wave == half)
    out_weight = jnp.where(single, 1.0, 2.0) / float(length) ** 2
    limits = jnp.where(valid, limit_ref[my_quarter], -1)
    order = order_ref[my_slab]
    strength = strength_ref[my_slab]
    wave_float = wave.astype(jnp.float32)

    @pl.loop(0, wav)
    def _(m):
        row = lax.broadcasted_iota(jnp.int32, (padded, 1), 0)
        q = row * wav + m
        signed_q = jnp.where(q < half, q, q - length)
        radius = (wave_float**2 + signed_q.astype(jnp.float32) ** 2) / (0.5 * length) ** 2
        square = radius * radius
        powered = jnp.where(order >= 3, square, 1.0) * jnp.where(order % 2 == 1, radius, square)
        inside = (jnp.abs(signed_q) <= limits) & (row < rows)
        damp[m] = jnp.where(inside, out_weight / (1.0 + strength * powered), 0.0)
        work[m, rows:] = jnp.zeros((padded - rows, 2 * wide), jnp.float32)

    @pl.loop(0, quarters)
    def _(quarter):
        @pl.loop(0, wide // 16)
        def _(block):
            at = quarter * (wide // 16) + block
            cos_c, sin_c = back_coarse[0, pl.ds(at, 1)], back_coarse[1, pl.ds(at, 1)]
            cos_f, sin_f = back_fine[0], back_fine[1]
            for part, value in enumerate((cos_c * cos_f - sin_c * sin_f, -(sin_c * cos_f + cos_c * sin_f))):
                span = pl.ds(pl.multiple_of(part * wide + block * 16, 16), 16)
                value_high, value_low = halves(value)
                back_table[quarter, 0, span] = value_high
                back_table[quarter, 1, span] = value_low

    out_ref[...] = jnp.zeros_like(out_ref)

    @pl.loop(0, wav)
    def _(w):
        arrive(sent, got, send_sems, recv_sems, w, local_sems.at[0])
        packed = got[w, 2 * rows :]
        for group, at, part, start, count in layout:
            piece = packed[at : at + count]
            rest[w, part, start : start + count] = pltpu.roll(piece, LANES - group * tail, 1) if group else piece

    @pl.loop(0, rows // 8)
    def _(block):
        span = pl.ds(pl.multiple_of(block * 8, 8), 8)
        under = pl.ds(pl.multiple_of(rows + block * 8, 8), 8)
        for tile in range(2):
            if tile == 0:
                x = [(got[w, span], got[w, under]) for w in range(wav)]
            else:
                x = [(rest[w, 0, span], rest[w, 1, span]) for w in range(wav)]
            for m, value in enumerate(eight_points(x, -1)):
                for part in range(2):
                    first = part * wide + tile * LANES
                    work[m, span, first : first + LANES] = value[part]

    base_parts = (base[0], base[1])

    def one_residue(m, sums):
        cos_t = jnp.concatenate([twiddle[0, m]] * 2, 1)
        sin_t = jnp.concatenate([twiddle[1, m]] * 2, 1)
        real, imag = work[m, :, :wide], work[m, :, wide:]
        turned = jnp.concatenate([real * cos_t + imag * sin_t, imag * cos_t - real * sin_t], 1)
        both = product(base_parts, halves(turned))
        factor = damp[m]
        real = (both[:padded, :wide] + both[padded:, wide:]) * factor
        imag = (both[:padded, wide:] - both[padded:, :wide]) * factor
        power = real * real + imag * imag
        sums = sums + jnp.sum(power.reshape(padded // 8, 8, wide), axis=0)
        both = product(base_parts, halves(jnp.concatenate([real, imag], 1)))
        real = both[:padded, :wide] - both[padded:, wide:]
        imag = both[:padded, wide:] + both[padded:, :wide]
        work[m, :, :wide] = real * cos_t - imag * sin_t
        work[m, :, wide:] = imag * cos_t + real * sin_t
        return sums

    sums = lax.fori_loop(0, wav, one_residue, jnp.zeros((8, wide), jnp.float32))
    sums = sums * jnp.where(single, 1.0, 0.5)
    sums = sums[:, :LANES] + sums[:, LANES:]
    energy_mine[0] = sums
    energy_mine[1] = sums * mass_ref[my_slab]

    @pl.loop(0, rows // 8)
    def _(block):
        span = pl.ds(pl.multiple_of(block * 8, 8), 8)
        under = pl.ds(pl.multiple_of(rows + block * 8, 8), 8)
        for tile in range(2):
            v = []
            for m in range(wav):
                first = tile * LANES
                v.append((work[m, span, first : first + LANES], work[m, span, wide + first : wide + first + LANES]))
            for w, value in enumerate(eight_points(v, 1)):
                if tile == 0:
                    sent_back[w, span] = value[0]
                    sent_back[w, under] = value[1]
                else:
                    rest[w, 0, span] = value[0]
                    rest[w, 1, span] = value[1]

    @pl.loop(0, quarters)
    def _(step):
        quarter = quarter_of(step)
        for slab in range(slabs):
            w = quarter * slabs + slab
            shifted = {}
            for group, at, part, start, count in layout:
                piece = rest[w, part, start : start + count]
                shifted.setdefault(group, []).append(pltpu.roll(piece, group * tail, 1) if group else piece)
            packed = jnp.zeros((group_rows, LANES), jnp.float32)
            for group, found in shifted.items():
                whole = jnp.concatenate(found, 0) if len(found) > 1 else found[0]
                if whole.shape[0] < group_rows:
                    fill = jnp.zeros((group_rows - whole.shape[0], LANES), jnp.float32)
                    whole = jnp.concatenate([whole, fill], 0)
                packed = packed + whole
            sent_back[w, 2 * rows :] = packed
            push(sent_back, got_back, back_send_sems, back_recv_sems, w, local_sems.at[1])

    def energy_copy(target_flat, slot):
        return pltpu.make_async_remote_copy(
            src_ref=energy_mine, dst_ref=energy_all.at[slot],
            send_sem=e_send_sems.at[target_flat], recv_sem=e_recv_sems.at[slot],
            device_id=(target_flat // wav, target_flat % wav), device_id_type=MESH,
        )

    @pl.loop(1, everyone)
    def _(step):
        energy_copy((flat + step) % everyone, flat).start()

    own_energy = pltpu.make_async_copy(energy_mine, energy_all.at[flat], local_sems.at[2])
    own_energy.start()

    @pl.loop(0, quarters)
    def _(step):
        quarter = quarter_of((step + quarters - 1) % quarters)
        stacked = []
        for slab in range(slabs):
            w = quarter * slabs + slab
            arrive(sent_back, got_back, back_send_sems, back_recv_sems, w, local_sems.at[1])
            packed = got_back[w, 2 * rows :]
            found = {0: [], 1: []}
            for group, at, part, start, count in layout:
                piece = packed[at : at + count]
                piece = pltpu.roll(piece, LANES - group * tail, 1) if group else piece
                found[part].append(jnp.where(lane < tail, piece, 0.0))
            stacked.append(
                jnp.concatenate(
                    [
                        got_back[w, :rows],
                        jnp.concatenate(found[0], 0),
                        got_back[w, rows : 2 * rows],
                        jnp.concatenate(found[1], 0),
                    ],
                    1,
                )
            )
        left = halves(jnp.concatenate(stacked, 0))
        out_ref[...] += product(left, (back_table[quarter, 0], back_table[quarter, 1]))

    own_energy.wait()

    @pl.loop(1, everyone)
    def _(step):
        source = (flat + step) % everyone
        energy_copy(source, source).wait()

    total = energy_all[0, 1]
    for n in range(1, everyone):
        total = total + energy_all[n, 1]
    total_ref[...] = jnp.full((1, LANES), jnp.sum(total) / (lev * slabs), jnp.float32)
    for slab in range(slabs):
        tile = energy_all[level * wav + slab, 0]
        for quarter in range(1, quarters):
            tile = tile + energy_all[level * wav + quarter * slabs + slab, 0]
        energy_ref[slab : slab + 1] = jnp.full((1, LANES), jnp.sum(tile), jnp.float32)


def cos_sin(phases, length):
    angles = 2.0 * np.pi / length * (phases % length)
    return np.stack([np.cos(angles), np.sin(angles)])


def fused(grid_field, truncation_limit, diffusion_order, diffusion_strength, mass_weight):
    slabs, rows, length = grid_field.shape
    wav, lev = lax.axis_size("wav"), lax.axis_size("lev")
    quarters = wav // slabs
    columns = length // 2 // quarters
    tail = columns + 1 - LANES
    groups = LANES // tail
    group_rows = -(-(-(-2 * rows // groups)) // 8) * 8
    padded = -(-rows // 16) * 16
    wide = 2 * LANES
    sizes = (slabs, rows, length, wav, lev, quarters, columns, padded, tail, groups, group_rows)
    starts = np.arange(quarters) * columns
    waves = starts[:, None] + np.arange(wide)[None]
    blocks = np.arange(length // 16) * 16
    sixteen = np.arange(16)
    positions = np.arange(length)
    single = lambda array: jnp.asarray(array, jnp.float32)
    coarse = single(cos_sin(blocks[None, :, None] * waves[:, None, :], length))
    fine = single(cos_sin(sixteen[None, :, None] * waves[:, None, :], length))
    back_starts = (starts[:, None] + np.arange(wide // 16)[None] * 16).reshape(-1)
    back_coarse = single(cos_sin(back_starts[:, None] * positions[None], length))
    back_fine = single(cos_sin(sixteen[:, None] * positions[None], length))
    inner = np.arange(padded)
    spread = np.zeros((1, 1, LANES), np.int64)
    twiddle = single(cos_sin(np.arange(wav)[:, None, None] * inner[None, :, None] + spread, length))
    base_exact = cos_sin(wav * inner[:, None] * inner[None], length)
    base_exact = base_exact * ((inner[:, None] < rows) & (inner[None] < rows))
    base_exact = base_exact.reshape(2 * padded, padded).astype(np.float32)
    base_high = base_exact.astype(jnp.bfloat16)
    base_low = (base_exact - base_high.astype(np.float32)).astype(jnp.bfloat16)
    base = jnp.asarray(np.stack([base_high, base_low]))
    limits = jnp.stack([truncation_limit[None, start : start + wide] for start in starts.tolist()])
    packed_rows = 2 * rows + group_rows
    everyone = wav * lev
    vmem, smem, anywhere = (pl.BlockSpec(memory_space=m) for m in (pltpu.VMEM, pltpu.SMEM, pl.ANY))
    f32, bf16 = jnp.float32, jnp.bfloat16
    filtered, energies, total = pl.pallas_call(
        functools.partial(fused_kernel, sizes),
        out_shape=(
            jax.ShapeDtypeStruct((slabs * rows, length), f32),
            jax.ShapeDtypeStruct((slabs, LANES), f32),
            jax.ShapeDtypeStruct((1, LANES), f32),
        ),
        in_specs=[vmem, vmem, smem, smem, smem, vmem, vmem] + [anywhere] * 4,
        out_specs=(vmem, vmem, vmem),
        scratch_shapes=[
            pltpu.VMEM((2, slabs * rows, length), bf16),
            pltpu.VMEM((2, length, 2 * wide), bf16),
            pltpu.VMEM((quarters, 2, 2 * wide, length), bf16),
            pltpu.VMEM(back_coarse.shape, f32),
            pltpu.VMEM(back_fine.shape, f32),
            pltpu.VMEM(twiddle.shape, f32),
            pltpu.VMEM(base.shape, bf16),
            pltpu.VMEM((wav, packed_rows, LANES), f32),
            pltpu.VMEM((wav, packed_rows, LANES), f32),
            pltpu.VMEM((wav, packed_rows, LANES), f32),
            pltpu.VMEM((wav, packed_rows, LANES), f32),
            pltpu.VMEM((wav, 2, rows, LANES), f32),
            pltpu.VMEM((wav, padded, 2 * wide), f32),
            pltpu.VMEM((wav, padded, wide), f32),
            pltpu.VMEM((2, 8, LANES), f32),
            pltpu.VMEM((everyone, 2, 8, LANES), f32),
            pltpu.SemaphoreType.DMA((4,)),
            pltpu.SemaphoreType.DMA((wav,)),
            pltpu.SemaphoreType.DMA((wav,)),
            pltpu.SemaphoreType.DMA((wav,)),
            pltpu.SemaphoreType.DMA((wav,)),
            pltpu.SemaphoreType.DMA((everyone,)),
            pltpu.SemaphoreType.DMA((everyone,)),
            pltpu.SemaphoreType.DMA((3,)),
        ],
        compiler_params=pltpu.CompilerParams(
            collective_id=0, has_side_effects=True, vmem_limit_bytes=60 * 1024 * 1024
        ),
        name="fused_step",
    )(
        grid_field.reshape(slabs * rows, length), limits, diffusion_order, diffusion_strength, mass_weight,
        coarse, fine, back_coarse, back_fine, twiddle, base,
    )
    return filtered.reshape(slabs, rows, length), energies[:, 0], total[0, 0]


def fits(shape):
    slabs, rows, length = shape
    wav = lax.axis_size("wav")
    if wav != 8 or slabs != 2 or rows % 8 or length % 16 or length != rows * wav:
        return False
    columns = length * slabs // 2 // wav
    return LANES <= columns < LANES + LANES // 2


def local(grid_field, truncation_limit, diffusion_order, diffusion_strength, mass_weight):
    slab_count, row_count, length = grid_field.shape
    if fits(grid_field.shape):
        return fused(
            grid_field, truncation_limit, diffusion_order, diffusion_strength, mass_weight
        )
    cosine_table, sine_table = tables(length)
    filtered, partial_value = half_plane(
        grid_field, truncation_limit, diffusion_order, diffusion_strength, cosine_table, sine_table
    )
    total_slabs = lax.axis_size("lev") * slab_count
    energies = lax.psum(partial_value, "wav")
    weighted_sum = lax.psum(jnp.sum(mass_weight * energies), "lev")
    total_energy = weighted_sum / total_slabs
    return (filtered, energies, total_energy)


def solution(mesh):
    placed = (P("lev", "wav", None), P(), P("lev"), P("lev"), P("lev"))
    return jax.shard_map(
        local,
        mesh=mesh,
        in_specs=placed,
        out_specs=(P("lev", "wav", None), P("lev"), P()),
        check_vma=False,
    )
```

```python
import functools

import jax
import jax.numpy as jnp
import numpy as np
from jax import lax
from jax.experimental import pallas as pl
from jax.experimental.pallas import tpu as pltpu
from jax.sharding import PartitionSpec as P

product_precision = lax.Precision.HIGH


def tables(length):
    step = 32
    coarse = -(-length // step)
    columns = np.arange(length)
    high = 2.0 * np.pi / length * (np.arange(coarse)[:, None] * step * columns[None, :] % length)
    low = 2.0 * np.pi / length * (np.arange(step)[:, None] * columns[None, :] % length)
    cos_high, sin_high = (jnp.asarray(f(high), jnp.float32)[:, None] for f in (np.cos, np.sin))
    cos_low, sin_low = (jnp.asarray(f(low), jnp.float32)[None] for f in (np.cos, np.sin))
    cosine = cos_high * cos_low - sin_high * sin_low
    sine = sin_high * cos_low + cos_high * sin_low
    return tuple(t.reshape(coarse * step, length)[:length] for t in (cosine, sine))


def signed(positions, length):
    return jnp.where(positions < length // 2, positions, positions - length)


def transform(values, cosine_table, sine_table, direction):
    with_cosine = jnp.einsum("scpi,iq->scpq", values, cosine_table, precision=product_precision)
    with_sine = jnp.einsum("scpi,iq->scpq", values, sine_table, precision=product_precision)
    if direction < 0:
        real_part = with_cosine[:, 0] + with_sine[:, 1]
        imaginary = with_cosine[:, 1] - with_sine[:, 0]
    else:
        real_part = with_cosine[:, 0] - with_sine[:, 1]
        imaginary = with_cosine[:, 1] + with_sine[:, 0]
    return jnp.stack([real_part, imaginary], axis=1)


def damping(wave_rows, limits, length, diffusion_order, diffusion_strength):
    wave_first = signed(jnp.arange(length, dtype=jnp.int32), length)
    rows_float = wave_rows.astype(jnp.float32)
    first_float = wave_first.astype(jnp.float32)
    scaled_radius = (rows_float[:, None] ** 2 + first_float[None, :] ** 2) / (0.5 * length) ** 2
    inside = (jnp.abs(wave_first)[None, :] <= limits[:, None]).astype(jnp.float32)
    powered = jnp.power(scaled_radius[None], diffusion_order.astype(jnp.float32)[:, None, None])
    return inside[None] / (1.0 + diffusion_strength[:, None, None] * powered)


def mirrored(values):
    return jnp.roll(jnp.flip(values, -1), 1, -1)


def half_plane(
    grid_field, truncation_limit, diffusion_order, diffusion_strength, cosine_table, sine_table
):
    length = grid_field.shape[2]
    half = length // 2
    row_real = jnp.einsum("sij,jl->sli", grid_field, cosine_table[:, :half], precision=product_precision)
    row_imag = -jnp.einsum("sij,jl->sli", grid_field, sine_table[:, :half], precision=product_precision)
    nyquist = jnp.einsum("sij,j->si", grid_field, cosine_table[:, half], precision=product_precision)
    zero_row = (jnp.arange(half, dtype=jnp.int32) == 0)[None, :, None]
    row_imag = jnp.where(zero_row, nyquist[:, None, :], row_imag)
    along_rows = jnp.stack([row_real, row_imag], axis=1)
    spectrum = transform(
        lax.all_to_all(along_rows, "wav", split_axis=2, concat_axis=3, tiled=True),
        cosine_table,
        sine_table,
        -1,
    )
    column_count = spectrum.shape[2]
    wav_index = lax.axis_index("wav")
    offset = wav_index * column_count
    wave_rows = offset + jnp.arange(column_count, dtype=jnp.int32)
    limits = lax.dynamic_slice(truncation_limit, (offset,), (column_count,))
    damp_main = damping(wave_rows, limits, length, diffusion_order, diffusion_strength)
    nyquist_rows = signed(jnp.full((1,), half, jnp.int32), length)
    damp_top = damping(
        nyquist_rows, truncation_limit[half : half + 1], length, diffusion_order, diffusion_strength
    )[:, 0]
    damped = spectrum * damp_main[:, None]
    packed_real = spectrum[:, 0, 0, :]
    packed_imag = spectrum[:, 1, 0, :]
    back_real = mirrored(packed_real)
    back_imag = mirrored(packed_imag)
    zero_real = (packed_real + back_real) * 0.5 * damp_main[:, 0]
    zero_imag = (packed_imag - back_imag) * 0.5 * damp_main[:, 0]
    top_real = (packed_imag + back_imag) * 0.5 * damp_top
    top_imag = (back_real - packed_real) * 0.5 * damp_top
    is_zero = wave_rows == 0
    column_weight = jnp.where(is_zero, 0.0, 2.0).astype(jnp.float32)
    edge = jnp.sum(zero_real**2 + zero_imag**2 + top_real**2 + top_imag**2, axis=-1)
    main_sum = jnp.sum(damped * damped * column_weight[None, None, :, None], axis=(1, 2, 3))
    partial_value = (main_sum + jnp.where(wav_index == 0, edge, 0.0)) / float(length) ** 4
    zero_column = is_zero[None, :, None]
    repacked = jnp.stack(
        [
            jnp.where(zero_column, (zero_real - top_imag)[:, None, :], damped[:, 0]),
            jnp.where(zero_column, (zero_imag + top_real)[:, None, :], damped[:, 1]),
        ],
        axis=1,
    )
    along_first = transform(repacked, cosine_table, sine_table, 1)
    inverse_area = 1.0 / float(length) ** 2
    received = lax.all_to_all(along_first, "wav", split_axis=3, concat_axis=2, tiled=True)
    row_weight = jnp.where(jnp.arange(half, dtype=jnp.int32) == 0, 1.0, 2.0).astype(jnp.float32)[
        :, None
    ]
    with_cosine = jnp.einsum(
        "spi,pj->sij", received[:, 0] * row_weight, cosine_table[:half], precision=product_precision
    )
    with_sine = jnp.einsum(
        "spi,pj->sij", received[:, 1] * row_weight, sine_table[:half], precision=product_precision
    )
    top_term = received[:, 1, 0, :][:, :, None] * cosine_table[half][None, None, :]
    filtered = (with_cosine - with_sine + top_term) * inverse_area
    return (filtered, partial_value)


LANES = 128
HALF = LANES // 2
MESH = pl.DeviceIdType.MESH


def halves(values):
    high = values.astype(jnp.bfloat16)
    return high, (values - high.astype(jnp.float32)).astype(jnp.bfloat16)


def product(left, right):
    dot = functools.partial(jnp.dot, preferred_element_type=jnp.float32)
    return dot(left[0], right[0]) + dot(left[1], right[0]) + dot(left[0], right[1])


def swap(value):
    count = value.shape[1] // LANES
    turned = [pltpu.roll(value[:, n * LANES : (n + 1) * LANES], HALF, 1) for n in range(count)]
    return jnp.concatenate(turned, 1) if count > 1 else turned[0]


def eight_points(x, sign, signs):
    turn = signs if sign < 0 else -signs

    def four(p, q, r, t):
        a0, a1, a2, a3 = p + r, p - r, q + t, swap(q - t) * turn
        return a0 + a2, a1 + a3, a0 - a2, a1 - a3

    e = four(x[0], x[2], x[4], x[6])
    o = four(x[1], x[3], x[5], x[7])
    root = 0.5**0.5
    odd = (
        o[0],
        root * (o[1] + swap(o[1]) * turn),
        swap(o[2]) * turn,
        root * (swap(o[3]) * turn - o[3]),
    )
    return [e[n] + odd[n] for n in range(4)] + [e[n] - odd[n] for n in range(4)]


def pieces(rows, group_rows, groups):
    found = []
    for group in range(groups):
        start, stop = group * group_rows, min((group + 1) * group_rows, 2 * rows)
        while start < stop:
            part = start // rows
            end = min(stop, (part + 1) * rows)
            found.append((group, start - group * group_rows, part, start - part * rows, end - start))
            start = end
    return found


def fused_kernel(
    sizes,
    grid_ref, limit_ref, order_ref, strength_ref, mass_ref, coarse_ref, fine_ref,
    back_coarse_hbm, back_fine_hbm, twiddle_hbm, base_hbm,
    out_ref, energy_ref, total_ref,
    grid_parts, table, back_table, back_coarse, back_fine, twiddle, base,
    sent_a, got_a, sent_b, got_b, back_a, home_a, back_b, home_b,
    rest, work, damp, energy_mine, energy_all,
    load_sems, send_sems, recv_sems, e_send_sems, e_recv_sems, local_sems,
):
    slabs, rows, length, wav, lev, quarters, columns, padded, tail, groups, group_rows, fine_rows = sizes
    everyone = lev * wav
    half = length // 2
    me = lax.axis_index("wav")
    level = lax.axis_index("lev")
    my_quarter, my_slab = me // slabs, me % slabs
    flat = level * wav + me

    barrier = pltpu.get_barrier_semaphore()

    @pl.loop(1, everyone)
    def _(step):
        target = (flat + step) % everyone
        pl.semaphore_signal(barrier, inc=1, device_id=(target // wav, target % wav), device_id_type=MESH)

    loads = [
        pltpu.make_async_copy(src, dst, load_sems.at[n])
        for n, (src, dst) in enumerate(
            ((twiddle_hbm, twiddle), (base_hbm, base), (back_coarse_hbm, back_coarse), (back_fine_hbm, back_fine))
        )
    ]
    for load in loads:
        load.start()
    high, low = halves(grid_ref[...])
    grid_parts[0] = high
    grid_parts[1] = low

    def quarter_of(step):
        down, across = 1 - step % 2, 1 - step // 2
        y, x = my_quarter // 2, my_quarter % 2
        return (y + down - 2 * y * down) * 2 + (x + across - 2 * x * across)

    def push(source, target, phase, w):
        @pl.when(w != me)
        def _():
            pltpu.make_async_remote_copy(
                src_ref=source.at[w], dst_ref=target.at[me],
                send_sem=send_sems.at[phase, w], recv_sem=recv_sems.at[phase, me],
                device_id=(level, w), device_id_type=MESH,
            ).start()

        @pl.when(w == me)
        def _():
            pltpu.make_async_copy(source.at[w], target.at[w], local_sems.at[phase]).start()

    def arrive(source, target, phase, w):
        @pl.when(w != me)
        def _():
            pltpu.make_async_remote_copy(
                src_ref=source.at[w], dst_ref=target.at[w],
                send_sem=send_sems.at[phase, w], recv_sem=recv_sems.at[phase, w],
                device_id=(level, w), device_id_type=MESH,
            ).wait()

        @pl.when(w == me)
        def _():
            pltpu.make_async_copy(source.at[w], target.at[w], local_sems.at[phase]).wait()

    lane = lax.broadcasted_iota(jnp.int32, (1, LANES), 1)
    signs = jnp.where(lane < HALF, 1.0, -1.0)
    in_part = [(lane >= part * HALF) & (lane < part * HALF + tail) for part in range(2)]
    layout = pieces(rows, group_rows, groups)

    def pack(tile):
        shifted = {}
        for group, at, part, start, count in layout:
            piece = jnp.where(in_part[part], tile(start, count), 0.0)
            shift = (group * tail - part * HALF) % LANES
            shifted.setdefault(group, []).append(pltpu.roll(piece, shift, 1) if shift else piece)
        packed = jnp.zeros((group_rows, LANES), jnp.float32)
        for found in shifted.values():
            whole = jnp.concatenate(found, 0) if len(found) > 1 else found[0]
            if whole.shape[0] < group_rows:
                fill = jnp.zeros((group_rows - whole.shape[0], LANES), jnp.float32)
                whole = jnp.concatenate([whole, fill], 0)
            packed = packed + whole
        return packed

    def unpack(packed):
        found = {0: [], 1: []}
        for group, at, part, start, count in layout:
            piece = packed[at : at + count]
            shift = (part * HALF - group * tail) % LANES
            piece = pltpu.roll(piece, shift, 1) if shift else piece
            found[part].append(jnp.where(in_part[part], piece, 0.0))
        return jnp.concatenate(found[0], 0) + jnp.concatenate(found[1], 0)

    def forward(first, count, phase, source, target):
        @pl.loop(0, quarters)
        def _(step):
            quarter = quarter_of(step)
            columns_of = slice(first * LANES, (first + count) * LANES)
            cos_f, sin_f = fine_ref[0, quarter, :, columns_of], fine_ref[1, quarter, :, columns_of]

            @pl.loop(0, length // fine_rows, unroll=2)
            def _(block):
                cos_c = coarse_ref[0, quarter, pl.ds(block, 1)][:, columns_of]
                sin_c = coarse_ref[1, quarter, pl.ds(block, 1)][:, columns_of]
                span = pl.ds(pl.multiple_of(block * fine_rows, fine_rows), fine_rows)
                value_high, value_low = halves(cos_c * cos_f - sin_c * sin_f)
                table[0, span, : count * LANES] = value_high
                table[1, span, : count * LANES] = value_low

            result = product(
                (grid_parts[0], grid_parts[1]), (table[0, :, : count * LANES], table[1, :, : count * LANES])
            )
            for slab in range(slabs):
                w = quarter * slabs + slab
                source[w, :rows] = result[slab * rows : (slab + 1) * rows, :LANES]
                if count > 1:
                    source[w, rows:] = pack(
                        lambda start, many: result[slab * rows + start : slab * rows + start + many, LANES:]
                    )

            if first == 0:
                @pl.when(step == 0)
                def _():
                    pl.semaphore_wait(barrier, everyone - 1)

            for slab in range(slabs):
                push(source, target, phase, quarter * slabs + slab)

    forward(0, 1, 0, sent_a, got_a)
    forward(1, 2, 1, sent_b, got_b)

    loads[0].wait()
    loads[1].wait()
    place = lax.broadcasted_iota(jnp.int32, (1, 3 * LANES), 1)
    column = place // LANES * HALF + place % HALF
    wave = my_quarter * columns + column
    valid = (column < columns) | ((column == columns) & (wave == half))
    single = (wave == 0) | (wave == half)
    out_weight = jnp.where(single, 1.0, 2.0) / float(length) ** 2
    energy_weight = jnp.where(single, 1.0, 0.5)
    limits = jnp.where(valid, limit_ref[my_quarter], -1)
    order = order_ref[my_slab]
    strength = strength_ref[my_slab]
    wave_square = wave.astype(jnp.float32) ** 2

    @pl.loop(0, wav)
    def _(m):
        row = lax.broadcasted_iota(jnp.int32, (padded, 1), 0)
        q = row * wav + m
        signed_q = jnp.where(q < half, q, q - length)
        radius = (wave_square + signed_q.astype(jnp.float32) ** 2) / (0.5 * length) ** 2
        square = radius * radius
        powered = jnp.where(order >= 3, square, 1.0) * jnp.where(order % 2 == 1, radius, square)
        inside = (jnp.abs(signed_q) <= limits) & (row < rows)
        damp[m] = jnp.where(inside, out_weight / (1.0 + strength * powered), 0.0)
        work[m, rows:] = jnp.zeros((padded - rows, 2 * LANES), jnp.float32)

    base_parts = (base[0], base[1])

    def middle(first, count, phase, got, back, home):
        spans = slice(0, count * LANES)
        all_signs = jnp.concatenate([signs] * count, 1)

        @pl.loop(0, rows // 8)
        def _(block):
            span = pl.ds(pl.multiple_of(block * 8, 8), 8)
            for tile in range(count):
                x = [rest[w, span] if tile else got[w, span] for w in range(wav)]
                for m, value in enumerate(eight_points(x, -1, signs)):
                    work[m, span, tile * LANES : (tile + 1) * LANES] = value

        def one_residue(m, sums):
            cos_t = jnp.concatenate([twiddle[0, m]] * count, 1)
            sin_t = jnp.concatenate([twiddle[1, m]] * count, 1)
            value = work[m, :, spans]
            both = product(base_parts, halves(value * cos_t + swap(value) * sin_t))
            value = both[:padded] + swap(both[padded:]) * all_signs
            value = value * damp[m, :, first * LANES : (first + count) * LANES]
            sums = sums + jnp.sum((value * value).reshape(padded // 8, 8, count * LANES), axis=0)
            both = product(base_parts, halves(value))
            value = both[:padded] - swap(both[padded:]) * all_signs
            work[m, :, spans] = value * cos_t - swap(value) * sin_t
            return sums

        sums = lax.fori_loop(0, wav, one_residue, jnp.zeros((8, count * LANES), jnp.float32), unroll=2)
        sums = sums * energy_weight[:, first * LANES : (first + count) * LANES]

        @pl.loop(0, rows // 8)
        def _(block):
            span = pl.ds(pl.multiple_of(block * 8, 8), 8)
            for tile in range(count):
                v = [work[m, span, tile * LANES : (tile + 1) * LANES] for m in range(wav)]
                for w, value in enumerate(eight_points(v, 1, signs)):
                    if tile:
                        rest[w, span] = value
                    else:
                        back[w, span] = value

        @pl.loop(0, quarters)
        def _(step):
            for slab in range(slabs):
                w = quarter_of(step) * slabs + slab
                if count > 1:
                    back[w, rows:] = pack(lambda start, many: rest[w, start : start + many])
                push(back, home, phase, w)

        return sum(sums[:, n * LANES : (n + 1) * LANES] for n in range(count))

    @pl.loop(0, wav)
    def _(w):
        arrive(sent_a, got_a, 0, w)

    sums = middle(0, 1, 2, got_a, back_a, home_a)

    loads[2].wait()
    loads[3].wait()
    blocks = 3 * LANES // fine_rows

    @pl.loop(0, quarters)
    def _(quarter):
        @pl.loop(0, blocks)
        def _(block):
            at = quarter * blocks + block
            cos_c, sin_c = back_coarse[0, pl.ds(at, 1)], back_coarse[1, pl.ds(at, 1)]
            span = pl.ds(pl.multiple_of(block * fine_rows, fine_rows), fine_rows)
            value_high, value_low = halves(cos_c * back_fine[0] - sin_c * back_fine[1])
            back_table[quarter, 0, span] = value_high
            back_table[quarter, 1, span] = value_low

    out_ref[...] = jnp.zeros_like(out_ref)

    @pl.loop(0, wav)
    def _(w):
        arrive(sent_b, got_b, 1, w)
        rest[w] = unpack(got_b[w, rows:])

    sums = sums + middle(1, 2, 3, got_b, back_b, home_b)
    energy_mine[0] = sums
    energy_mine[1] = sums * mass_ref[my_slab]

    def energy_copy(target_flat, slot):
        return pltpu.make_async_remote_copy(
            src_ref=energy_mine, dst_ref=energy_all.at[slot],
            send_sem=e_send_sems.at[target_flat], recv_sem=e_recv_sems.at[slot],
            device_id=(target_flat // wav, target_flat % wav), device_id_type=MESH,
        )

    @pl.loop(1, everyone)
    def _(step):
        energy_copy((flat + step) % everyone, flat).start()

    own_energy = pltpu.make_async_copy(energy_mine, energy_all.at[flat], local_sems.at[4])
    own_energy.start()

    def finish(first, count, phase, back, home):
        @pl.loop(0, quarters)
        def _(step):
            quarter = quarter_of((step + quarters - 1) % quarters)
            stacked = []
            for slab in range(slabs):
                w = quarter * slabs + slab
                arrive(back, home, phase, w)
                tiles = [home[w, :rows]]
                if count > 1:
                    tiles.append(unpack(home[w, rows:]))
                stacked.append(jnp.concatenate(tiles, 1) if count > 1 else tiles[0])
            left = halves(jnp.concatenate(stacked, 0))
            span = slice(first * LANES, (first + count) * LANES)
            out_ref[...] += product(left, (back_table[quarter, 0, span], back_table[quarter, 1, span]))

    finish(0, 1, 2, back_a, home_a)
    finish(1, 2, 3, back_b, home_b)
    own_energy.wait()

    @pl.loop(1, everyone)
    def _(step):
        source = (flat + step) % everyone
        energy_copy(source, source).wait()

    total = energy_all[0, 1]
    for n in range(1, everyone):
        total = total + energy_all[n, 1]
    total_ref[0] = jnp.sum(total) / (lev * slabs)
    for slab in range(slabs):
        tile = energy_all[level * wav + slab, 0]
        for quarter in range(1, quarters):
            tile = tile + energy_all[level * wav + quarter * slabs + slab, 0]
        energy_ref[slab] = jnp.sum(tile)


def cos_sin(phases, length):
    angles = 2.0 * np.pi / length * (phases % length)
    return np.stack([np.cos(angles), np.sin(angles)])


def fused(grid_field, truncation_limit, diffusion_order, diffusion_strength, mass_weight):
    slabs, rows, length = grid_field.shape
    wav, lev = lax.axis_size("wav"), lax.axis_size("lev")
    quarters = wav // slabs
    columns = length // 2 // quarters
    tail = columns + 1 - LANES
    groups = LANES // tail
    group_rows = -(-(-(-2 * rows // groups)) // 8) * 8
    padded = -(-rows // 16) * 16
    fine_rows = 32
    sizes = (slabs, rows, length, wav, lev, quarters, columns, padded, tail, groups, group_rows, fine_rows)
    starts = np.arange(quarters) * columns
    place = np.arange(3 * LANES)
    column = place // LANES * HALF + place % HALF
    phase = (place % LANES >= HALF) * (length // 4)
    waves = starts[:, None] + column[None]
    steps = np.arange(length // fine_rows) * fine_rows
    near = np.arange(fine_rows)
    positions = np.arange(length)
    single = lambda array: jnp.asarray(array, jnp.float32)
    coarse = single(cos_sin(steps[None, :, None] * waves[:, None, :], length))
    fine = single(cos_sin(near[None, :, None] * waves[:, None, :] + phase, length))
    back_starts = waves[:, ::fine_rows].reshape(-1)
    back_phase = np.tile(phase[::fine_rows], quarters)
    back_coarse = single(cos_sin(back_starts[:, None] * positions[None] + back_phase[:, None], length))
    back_fine = single(cos_sin(near[:, None] * positions[None], length))
    inner = np.arange(padded)
    spread = np.zeros((1, 1, LANES), np.int64)
    twiddle = cos_sin(np.arange(wav)[:, None, None] * inner[None, :, None] + spread, length)
    twiddle[1] *= np.where(np.arange(LANES) < HALF, 1.0, -1.0)
    twiddle = single(twiddle)
    base_exact = cos_sin(wav * inner[:, None] * inner[None], length)
    base_exact = base_exact * ((inner[:, None] < rows) & (inner[None] < rows))
    base_exact = base_exact.reshape(2 * padded, padded).astype(np.float32)
    base_high = base_exact.astype(jnp.bfloat16)
    base_low = (base_exact - base_high.astype(np.float32)).astype(jnp.bfloat16)
    base = jnp.asarray(np.stack([base_high, base_low]))
    tiles = [truncation_limit[start : start + HALF] for start in waves[:, ::LANES].reshape(-1).tolist()]
    limits = jnp.concatenate([tile for tile in tiles for _ in range(2)]).reshape(quarters, 1, 3 * LANES)
    chunk_a = pltpu.VMEM((wav, rows, LANES), jnp.float32)
    chunk_b = pltpu.VMEM((wav, rows + group_rows, LANES), jnp.float32)
    everyone = wav * lev
    vmem, smem, anywhere = (pl.BlockSpec(memory_space=m) for m in (pltpu.VMEM, pltpu.SMEM, pl.ANY))
    f32, bf16 = jnp.float32, jnp.bfloat16
    filtered, energies, total = pl.pallas_call(
        functools.partial(fused_kernel, sizes),
        out_shape=(
            jax.ShapeDtypeStruct((slabs * rows, length), f32),
            jax.ShapeDtypeStruct((slabs,), f32),
            jax.ShapeDtypeStruct((1,), f32),
        ),
        in_specs=[vmem, vmem, smem, smem, smem, vmem, vmem] + [anywhere] * 4,
        out_specs=(vmem, smem, smem),
        scratch_shapes=[
            pltpu.VMEM((2, slabs * rows, length), bf16),
            pltpu.VMEM((2, length, 2 * LANES), bf16),
            pltpu.VMEM((quarters, 2, 3 * LANES, length), bf16),
            pltpu.VMEM(back_coarse.shape, f32),
            pltpu.VMEM(back_fine.shape, f32),
            pltpu.VMEM(twiddle.shape, f32),
            pltpu.VMEM(base.shape, bf16),
            chunk_a, chunk_a, chunk_b, chunk_b, chunk_a, chunk_a, chunk_b, chunk_b,
            pltpu.VMEM((wav, rows, LANES), f32),
            pltpu.VMEM((wav, padded, 2 * LANES), f32),
            pltpu.VMEM((wav, padded, 3 * LANES), f32),
            pltpu.VMEM((2, 8, LANES), f32),
            pltpu.VMEM((everyone, 2, 8, LANES), f32),
            pltpu.SemaphoreType.DMA((4,)),
            pltpu.SemaphoreType.DMA((4, wav)),
            pltpu.SemaphoreType.DMA((4, wav)),
            pltpu.SemaphoreType.DMA((everyone,)),
            pltpu.SemaphoreType.DMA((everyone,)),
            pltpu.SemaphoreType.DMA((5,)),
        ],
        compiler_params=pltpu.CompilerParams(
            collective_id=0, has_side_effects=True, vmem_limit_bytes=60 * 1024 * 1024
        ),
        name="fused_step",
    )(
        grid_field.reshape(slabs * rows, length), limits, diffusion_order, diffusion_strength, mass_weight,
        coarse, fine, back_coarse, back_fine, twiddle, base,
    )
    return filtered.reshape(slabs, rows, length), energies, total[0]


def fits(shape):
    slabs, rows, length = shape
    wav = lax.axis_size("wav")
    if wav != 8 or slabs != 2 or rows % 8 or length % 16 or length != rows * wav:
        return False
    columns = length * slabs // 2 // wav
    return length % 32 == 0 and LANES <= columns < LANES + LANES // 2


def local(grid_field, truncation_limit, diffusion_order, diffusion_strength, mass_weight):
    slab_count, row_count, length = grid_field.shape
    if fits(grid_field.shape):
        return fused(
            grid_field, truncation_limit, diffusion_order, diffusion_strength, mass_weight
        )
    cosine_table, sine_table = tables(length)
    filtered, partial_value = half_plane(
        grid_field, truncation_limit, diffusion_order, diffusion_strength, cosine_table, sine_table
    )
    total_slabs = lax.axis_size("lev") * slab_count
    energies = lax.psum(partial_value, "wav")
    weighted_sum = lax.psum(jnp.sum(mass_weight * energies), "lev")
    total_energy = weighted_sum / total_slabs
    return (filtered, energies, total_energy)


def solution(mesh):
    placed = (P("lev", "wav", None), P(), P("lev"), P("lev"), P("lev"))
    return jax.shard_map(
        local,
        mesh=mesh,
        in_specs=placed,
        out_specs=(P("lev", "wav", None), P("lev"), P()),
        check_vma=False,
    )
```

```python
import functools

import jax
import jax.numpy as jnp
import numpy as np
from jax import lax
from jax.experimental import pallas as pl
from jax.experimental.pallas import tpu as pltpu
from jax.sharding import PartitionSpec as P

product_precision = lax.Precision.HIGH


def tables(length):
    step = 32
    coarse = -(-length // step)
    columns = np.arange(length)
    high = 2.0 * np.pi / length * (np.arange(coarse)[:, None] * step * columns[None, :] % length)
    low = 2.0 * np.pi / length * (np.arange(step)[:, None] * columns[None, :] % length)
    cos_high, sin_high = (jnp.asarray(f(high), jnp.float32)[:, None] for f in (np.cos, np.sin))
    cos_low, sin_low = (jnp.asarray(f(low), jnp.float32)[None] for f in (np.cos, np.sin))
    cosine = cos_high * cos_low - sin_high * sin_low
    sine = sin_high * cos_low + cos_high * sin_low
    return tuple(t.reshape(coarse * step, length)[:length] for t in (cosine, sine))


def signed(positions, length):
    return jnp.where(positions < length // 2, positions, positions - length)


def transform(values, cosine_table, sine_table, direction):
    with_cosine = jnp.einsum("scpi,iq->scpq", values, cosine_table, precision=product_precision)
    with_sine = jnp.einsum("scpi,iq->scpq", values, sine_table, precision=product_precision)
    if direction < 0:
        real_part = with_cosine[:, 0] + with_sine[:, 1]
        imaginary = with_cosine[:, 1] - with_sine[:, 0]
    else:
        real_part = with_cosine[:, 0] - with_sine[:, 1]
        imaginary = with_cosine[:, 1] + with_sine[:, 0]
    return jnp.stack([real_part, imaginary], axis=1)


def damping(wave_rows, limits, length, diffusion_order, diffusion_strength):
    wave_first = signed(jnp.arange(length, dtype=jnp.int32), length)
    rows_float = wave_rows.astype(jnp.float32)
    first_float = wave_first.astype(jnp.float32)
    scaled_radius = (rows_float[:, None] ** 2 + first_float[None, :] ** 2) / (0.5 * length) ** 2
    inside = (jnp.abs(wave_first)[None, :] <= limits[:, None]).astype(jnp.float32)
    powered = jnp.power(scaled_radius[None], diffusion_order.astype(jnp.float32)[:, None, None])
    return inside[None] / (1.0 + diffusion_strength[:, None, None] * powered)


def mirrored(values):
    return jnp.roll(jnp.flip(values, -1), 1, -1)


def half_plane(
    grid_field, truncation_limit, diffusion_order, diffusion_strength, cosine_table, sine_table
):
    length = grid_field.shape[2]
    half = length // 2
    row_real = jnp.einsum("sij,jl->sli", grid_field, cosine_table[:, :half], precision=product_precision)
    row_imag = -jnp.einsum("sij,jl->sli", grid_field, sine_table[:, :half], precision=product_precision)
    nyquist = jnp.einsum("sij,j->si", grid_field, cosine_table[:, half], precision=product_precision)
    zero_row = (jnp.arange(half, dtype=jnp.int32) == 0)[None, :, None]
    row_imag = jnp.where(zero_row, nyquist[:, None, :], row_imag)
    along_rows = jnp.stack([row_real, row_imag], axis=1)
    spectrum = transform(
        lax.all_to_all(along_rows, "wav", split_axis=2, concat_axis=3, tiled=True),
        cosine_table,
        sine_table,
        -1,
    )
    column_count = spectrum.shape[2]
    wav_index = lax.axis_index("wav")
    offset = wav_index * column_count
    wave_rows = offset + jnp.arange(column_count, dtype=jnp.int32)
    limits = lax.dynamic_slice(truncation_limit, (offset,), (column_count,))
    damp_main = damping(wave_rows, limits, length, diffusion_order, diffusion_strength)
    nyquist_rows = signed(jnp.full((1,), half, jnp.int32), length)
    damp_top = damping(
        nyquist_rows, truncation_limit[half : half + 1], length, diffusion_order, diffusion_strength
    )[:, 0]
    damped = spectrum * damp_main[:, None]
    packed_real = spectrum[:, 0, 0, :]
    packed_imag = spectrum[:, 1, 0, :]
    back_real = mirrored(packed_real)
    back_imag = mirrored(packed_imag)
    zero_real = (packed_real + back_real) * 0.5 * damp_main[:, 0]
    zero_imag = (packed_imag - back_imag) * 0.5 * damp_main[:, 0]
    top_real = (packed_imag + back_imag) * 0.5 * damp_top
    top_imag = (back_real - packed_real) * 0.5 * damp_top
    is_zero = wave_rows == 0
    column_weight = jnp.where(is_zero, 0.0, 2.0).astype(jnp.float32)
    edge = jnp.sum(zero_real**2 + zero_imag**2 + top_real**2 + top_imag**2, axis=-1)
    main_sum = jnp.sum(damped * damped * column_weight[None, None, :, None], axis=(1, 2, 3))
    partial_value = (main_sum + jnp.where(wav_index == 0, edge, 0.0)) / float(length) ** 4
    zero_column = is_zero[None, :, None]
    repacked = jnp.stack(
        [
            jnp.where(zero_column, (zero_real - top_imag)[:, None, :], damped[:, 0]),
            jnp.where(zero_column, (zero_imag + top_real)[:, None, :], damped[:, 1]),
        ],
        axis=1,
    )
    along_first = transform(repacked, cosine_table, sine_table, 1)
    inverse_area = 1.0 / float(length) ** 2
    received = lax.all_to_all(along_first, "wav", split_axis=3, concat_axis=2, tiled=True)
    row_weight = jnp.where(jnp.arange(half, dtype=jnp.int32) == 0, 1.0, 2.0).astype(jnp.float32)[
        :, None
    ]
    with_cosine = jnp.einsum(
        "spi,pj->sij", received[:, 0] * row_weight, cosine_table[:half], precision=product_precision
    )
    with_sine = jnp.einsum(
        "spi,pj->sij", received[:, 1] * row_weight, sine_table[:half], precision=product_precision
    )
    top_term = received[:, 1, 0, :][:, :, None] * cosine_table[half][None, None, :]
    filtered = (with_cosine - with_sine + top_term) * inverse_area
    return (filtered, partial_value)


LANES = 128
HALF = LANES // 2
MESH = pl.DeviceIdType.MESH


def halves(values):
    high = values.astype(jnp.bfloat16)
    return high, (values - high.astype(jnp.float32)).astype(jnp.bfloat16)


def product(left, right):
    dot = functools.partial(jnp.dot, preferred_element_type=jnp.float32)
    return dot(left[0], right[0]) + dot(left[1], right[0]) + dot(left[0], right[1])


def swap(value):
    count = value.shape[1] // LANES
    turned = [pltpu.roll(value[:, n * LANES : (n + 1) * LANES], HALF, 1) for n in range(count)]
    return jnp.concatenate(turned, 1) if count > 1 else turned[0]


def eight_points(x, sign, signs):
    turn = signs if sign < 0 else -signs

    def four(p, q, r, t):
        a0, a1, a2, a3 = p + r, p - r, q + t, swap(q - t) * turn
        return a0 + a2, a1 + a3, a0 - a2, a1 - a3

    e = four(x[0], x[2], x[4], x[6])
    o = four(x[1], x[3], x[5], x[7])
    root = 0.5**0.5
    odd = (
        o[0],
        root * (o[1] + swap(o[1]) * turn),
        swap(o[2]) * turn,
        root * (swap(o[3]) * turn - o[3]),
    )
    return [e[n] + odd[n] for n in range(4)] + [e[n] - odd[n] for n in range(4)]


def pieces(rows, group_rows, groups):
    found = []
    for group in range(groups):
        start, stop = group * group_rows, min((group + 1) * group_rows, 2 * rows)
        while start < stop:
            part = start // rows
            end = min(stop, (part + 1) * rows)
            found.append((group, start - group * group_rows, part, start - part * rows, end - start))
            start = end
    return found


def fused_kernel(
    sizes,
    grid_ref, limit_ref, order_ref, strength_ref, mass_ref, coarse_ref, fine_ref,
    back_coarse_hbm, back_fine_hbm, twiddle_hbm, base_hbm,
    out_ref, energy_ref, total_ref,
    grid_parts, table, back_table, back_coarse, back_fine, twiddle, base,
    sent_a, got_a, sent_b, got_b, back_a, home_a, back_b, home_b,
    rest, work, damp, energy_mine, energy_all,
    load_sems, send_sems, recv_sems, e_send_sems, e_recv_sems, local_sems,
):
    slabs, rows, length, wav, lev, quarters, columns, padded, tail, groups, group_rows, fine_rows = sizes
    everyone = lev * wav
    half = length // 2
    me = lax.axis_index("wav")
    level = lax.axis_index("lev")
    my_quarter, my_slab = me // slabs, me % slabs
    flat = level * wav + me

    barrier = pltpu.get_barrier_semaphore()

    @pl.loop(1, everyone)
    def _(step):
        target = (flat + step) % everyone
        pl.semaphore_signal(barrier, inc=1, device_id=(target // wav, target % wav), device_id_type=MESH)

    loads = [
        pltpu.make_async_copy(src, dst, load_sems.at[n])
        for n, (src, dst) in enumerate(
            ((twiddle_hbm, twiddle), (base_hbm, base), (back_coarse_hbm, back_coarse), (back_fine_hbm, back_fine))
        )
    ]
    for load in loads:
        load.start()
    high, low = halves(grid_ref[...])
    grid_parts[0] = high
    grid_parts[1] = low

    def quarter_of(step):
        down, across = 1 - step % 2, 1 - step // 2
        y, x = my_quarter // 2, my_quarter % 2
        return (y + down - 2 * y * down) * 2 + (x + across - 2 * x * across)

    def push(source, target, phase, w):
        @pl.when(w != me)
        def _():
            pltpu.make_async_remote_copy(
                src_ref=source.at[w], dst_ref=target.at[me],
                send_sem=send_sems.at[phase, w], recv_sem=recv_sems.at[phase, me],
                device_id=(level, w), device_id_type=MESH,
            ).start()

        @pl.when(w == me)
        def _():
            pltpu.make_async_copy(source.at[w], target.at[w], local_sems.at[phase]).start()

    def arrive(source, target, phase, w):
        @pl.when(w != me)
        def _():
            pltpu.make_async_remote_copy(
                src_ref=source.at[w], dst_ref=target.at[w],
                send_sem=send_sems.at[phase, w], recv_sem=recv_sems.at[phase, w],
                device_id=(level, w), device_id_type=MESH,
            ).wait()

        @pl.when(w == me)
        def _():
            pltpu.make_async_copy(source.at[w], target.at[w], local_sems.at[phase]).wait()

    lane = lax.broadcasted_iota(jnp.int32, (1, LANES), 1)
    signs = jnp.where(lane < HALF, 1.0, -1.0)
    in_part = [(lane >= part * HALF) & (lane < part * HALF + tail) for part in range(2)]
    layout = pieces(rows, group_rows, groups)

    def pack(tile):
        shifted = {}
        for group, at, part, start, count in layout:
            piece = jnp.where(in_part[part], tile(start, count), 0.0)
            shift = (group * tail - part * HALF) % LANES
            shifted.setdefault(group, []).append(pltpu.roll(piece, shift, 1) if shift else piece)
        packed = jnp.zeros((group_rows, LANES), jnp.float32)
        for found in shifted.values():
            whole = jnp.concatenate(found, 0) if len(found) > 1 else found[0]
            if whole.shape[0] < group_rows:
                fill = jnp.zeros((group_rows - whole.shape[0], LANES), jnp.float32)
                whole = jnp.concatenate([whole, fill], 0)
            packed = packed + whole
        return packed

    def unpack(packed):
        found = {0: [], 1: []}
        for group, at, part, start, count in layout:
            piece = packed[at : at + count]
            shift = (part * HALF - group * tail) % LANES
            piece = pltpu.roll(piece, shift, 1) if shift else piece
            found[part].append(jnp.where(in_part[part], piece, 0.0))
        return jnp.concatenate(found[0], 0) + jnp.concatenate(found[1], 0)

    def forward(first, count, phase, source, target):
        @pl.loop(0, quarters)
        def _(step):
            quarter = quarter_of(step)
            columns_of = slice(first * LANES, (first + count) * LANES)
            cos_f, sin_f = fine_ref[0, quarter, :, columns_of], fine_ref[1, quarter, :, columns_of]

            @pl.loop(0, length // fine_rows, unroll=2)
            def _(block):
                cos_c = coarse_ref[0, quarter, pl.ds(block, 1)][:, columns_of]
                sin_c = coarse_ref[1, quarter, pl.ds(block, 1)][:, columns_of]
                span = pl.ds(pl.multiple_of(block * fine_rows, fine_rows), fine_rows)
                value_high, value_low = halves(cos_c * cos_f - sin_c * sin_f)
                table[0, span, : count * LANES] = value_high
                table[1, span, : count * LANES] = value_low

            result = product(
                (grid_parts[0], grid_parts[1]), (table[0, :, : count * LANES], table[1, :, : count * LANES])
            )
            for slab in range(slabs):
                w = quarter * slabs + slab
                source[w, :rows] = result[slab * rows : (slab + 1) * rows, :LANES]
                if count > 1:
                    source[w, rows:] = pack(
                        lambda start, many: result[slab * rows + start : slab * rows + start + many, LANES:]
                    )

            if first == 0:
                @pl.when(step == 0)
                def _():
                    pl.semaphore_wait(barrier, everyone - 1)

            for slab in range(slabs):
                push(source, target, phase, quarter * slabs + slab)

    forward(0, 1, 0, sent_a, got_a)
    forward(1, 2, 1, sent_b, got_b)

    loads[0].wait()
    loads[1].wait()
    place = lax.broadcasted_iota(jnp.int32, (1, 3 * LANES), 1)
    column = place // LANES * HALF + place % HALF
    wave = my_quarter * columns + column
    valid = (column < columns) | ((column == columns) & (wave == half))
    single = (wave == 0) | (wave == half)
    out_weight = jnp.where(single, 1.0, 2.0) / float(length) ** 2
    energy_weight = jnp.where(single, 1.0, 0.5)
    all_limits = limit_ref[...]
    limits = jnp.full((1, 3 * LANES), -1, jnp.int32)
    for quarter in range(quarters):
        found = []
        for tile in range(3):
            start = quarter * columns + tile * HALF
            found += [all_limits[:, start : start + HALF]] * 2
        limits = jnp.where(my_quarter == quarter, jnp.concatenate(found, 1), limits)
    limits = jnp.where(valid, limits, -1)
    order = order_ref[my_slab]
    strength = strength_ref[my_slab]
    wave_square = wave.astype(jnp.float32) ** 2

    @pl.loop(0, wav)
    def _(m):
        row = lax.broadcasted_iota(jnp.int32, (padded, 1), 0)
        q = row * wav + m
        signed_q = jnp.where(q < half, q, q - length)
        radius = (wave_square + signed_q.astype(jnp.float32) ** 2) / (0.5 * length) ** 2
        square = radius * radius
        powered = jnp.where(order >= 3, square, 1.0) * jnp.where(order % 2 == 1, radius, square)
        inside = (jnp.abs(signed_q) <= limits) & (row < rows)
        damp[m] = jnp.where(inside, out_weight / (1.0 + strength * powered), 0.0)
        work[m, rows:] = jnp.zeros((padded - rows, 2 * LANES), jnp.float32)

    base_parts = (base[0], base[1])
    block_rows = 24

    def in_blocks(body):
        @pl.loop(0, rows // block_rows)
        def _(block):
            body(pl.multiple_of(block * block_rows, 8), block_rows)

        if rows % block_rows:
            body(rows - rows % block_rows, rows % block_rows)

    def middle(first, count, phase, got, back, home, announce):
        spans = slice(0, count * LANES)
        all_signs = jnp.concatenate([signs] * count, 1)

        def split(start, many):
            span = pl.ds(start, many)
            for tile in range(count):
                x = [rest[w, span] if tile else got[w, span] for w in range(wav)]
                for m, value in enumerate(eight_points(x, -1, signs)):
                    work[m, span, tile * LANES : (tile + 1) * LANES] = value

        in_blocks(split)

        def one_residue(m, sums):
            packed_turn = twiddle[m]
            other_turn = swap(packed_turn)
            cos_t = jnp.concatenate([jnp.where(lane < HALF, packed_turn, other_turn)] * count, 1)
            sin_t = jnp.concatenate([jnp.where(lane < HALF, other_turn, -packed_turn)] * count, 1)
            value = work[m, :, spans]
            both = product(base_parts, halves(value * cos_t + swap(value) * sin_t))
            value = both[:padded] + swap(both[padded:]) * all_signs
            value = value * damp[m, :, first * LANES : (first + count) * LANES]
            sums = sums + jnp.sum((value * value).reshape(padded // 8, 8, count * LANES), axis=0)
            both = product(base_parts, halves(value))
            value = both[:padded] - swap(both[padded:]) * all_signs
            work[m, :, spans] = value * cos_t - swap(value) * sin_t
            return sums

        sums = lax.fori_loop(0, wav, one_residue, jnp.zeros((8, count * LANES), jnp.float32), unroll=4)
        sums = sums * energy_weight[:, first * LANES : (first + count) * LANES]

        announce(sum(sums[:, n * LANES : (n + 1) * LANES] for n in range(count)))

        def join(start, many):
            span = pl.ds(start, many)
            for tile in range(count):
                v = [work[m, span, tile * LANES : (tile + 1) * LANES] for m in range(wav)]
                for w, value in enumerate(eight_points(v, 1, signs)):
                    if tile:
                        rest[w, span] = value
                    else:
                        back[w, span] = value

        in_blocks(join)

        @pl.loop(0, quarters)
        def _(step):
            for slab in range(slabs):
                w = quarter_of(step) * slabs + slab
                if count > 1:
                    back[w, rows:] = pack(lambda start, many: rest[w, start : start + many])
                push(back, home, phase, w)

    @pl.loop(0, wav)
    def _(w):
        arrive(sent_a, got_a, 0, w)

    def energy_copy(target_flat, slot):
        return pltpu.make_async_remote_copy(
            src_ref=energy_mine, dst_ref=energy_all.at[slot],
            send_sem=e_send_sems.at[target_flat], recv_sem=e_recv_sems.at[slot],
            device_id=(target_flat // wav, target_flat % wav), device_id_type=MESH,
        )

    def announce_first(sums):
        energy_mine[0] = sums

    def announce_last(sums):
        sums = sums + energy_mine[0]
        energy_mine[0] = sums
        energy_mine[1] = sums * mass_ref[my_slab]

        @pl.loop(1, everyone)
        def _(step):
            energy_copy((flat + step) % everyone, flat).start()

        pltpu.make_async_copy(energy_mine, energy_all.at[flat], local_sems.at[4]).start()

    middle(0, 1, 2, got_a, back_a, home_a, announce_first)

    loads[2].wait()
    loads[3].wait()
    blocks = 3 * LANES // fine_rows

    @pl.loop(0, quarters)
    def _(quarter):
        @pl.loop(0, blocks)
        def _(block):
            at = quarter * blocks + block
            cos_c, sin_c = back_coarse[0, pl.ds(at, 1)], back_coarse[1, pl.ds(at, 1)]
            span = pl.ds(pl.multiple_of(block * fine_rows, fine_rows), fine_rows)
            value_high, value_low = halves(cos_c * back_fine[0] - sin_c * back_fine[1])
            back_table[quarter, 0, span] = value_high
            back_table[quarter, 1, span] = value_low

    out_ref[...] = jnp.zeros_like(out_ref)

    @pl.loop(0, wav)
    def _(w):
        arrive(sent_b, got_b, 1, w)
        rest[w] = unpack(got_b[w, rows:])

    middle(1, 2, 3, got_b, back_b, home_b, announce_last)
    own_energy = pltpu.make_async_copy(energy_mine, energy_all.at[flat], local_sems.at[4])

    def finish(first, count, phase, back, home):
        @pl.loop(0, quarters)
        def _(step):
            quarter = quarter_of((step + quarters - 1) % quarters)
            stacked = []
            for slab in range(slabs):
                w = quarter * slabs + slab
                arrive(back, home, phase, w)
                tiles = [home[w, :rows]]
                if count > 1:
                    tiles.append(unpack(home[w, rows:]))
                stacked.append(jnp.concatenate(tiles, 1) if count > 1 else tiles[0])
            left = halves(jnp.concatenate(stacked, 0))
            span = slice(first * LANES, (first + count) * LANES)
            out_ref[...] += product(left, (back_table[quarter, 0, span], back_table[quarter, 1, span]))

    finish(0, 1, 2, back_a, home_a)
    finish(1, 2, 3, back_b, home_b)
    own_energy.wait()

    @pl.loop(1, everyone)
    def _(step):
        source = (flat + step) % everyone
        energy_copy(source, source).wait()

    total = energy_all[0, 1]
    for n in range(1, everyone):
        total = total + energy_all[n, 1]
    total_ref[0] = jnp.sum(total) / (lev * slabs)
    for slab in range(slabs):
        tile = energy_all[level * wav + slab, 0]
        for quarter in range(1, quarters):
            tile = tile + energy_all[level * wav + quarter * slabs + slab, 0]
        energy_ref[slab] = jnp.sum(tile)


def cos_sin(phases, length):
    angles = 2.0 * np.pi / length * (phases % length)
    return np.stack([np.cos(angles), np.sin(angles)])


def fused(grid_field, truncation_limit, diffusion_order, diffusion_strength, mass_weight):
    slabs, rows, length = grid_field.shape
    wav, lev = lax.axis_size("wav"), lax.axis_size("lev")
    quarters = wav // slabs
    columns = length // 2 // quarters
    tail = columns + 1 - LANES
    groups = LANES // tail
    group_rows = -(-(-(-2 * rows // groups)) // 8) * 8
    padded = -(-rows // 16) * 16
    fine_rows = 32
    sizes = (slabs, rows, length, wav, lev, quarters, columns, padded, tail, groups, group_rows, fine_rows)
    starts = np.arange(quarters) * columns
    place = np.arange(3 * LANES)
    column = place // LANES * HALF + place % HALF
    phase = (place % LANES >= HALF) * (length // 4)
    waves = starts[:, None] + column[None]
    steps = np.arange(length // fine_rows) * fine_rows
    near = np.arange(fine_rows)
    positions = np.arange(length)
    single = lambda array: jnp.asarray(array, jnp.float32)
    coarse = single(cos_sin(steps[None, :, None] * waves[:, None, :], length))
    fine = single(cos_sin(near[None, :, None] * waves[:, None, :] + phase, length))
    back_starts = waves[:, ::fine_rows].reshape(-1)
    back_phase = np.tile(phase[::fine_rows], quarters)
    back_coarse = single(cos_sin(back_starts[:, None] * positions[None] + back_phase[:, None], length))
    back_fine = single(cos_sin(near[:, None] * positions[None], length))
    inner = np.arange(padded)
    turns = cos_sin(np.arange(wav)[:, None, None] * inner[None, :, None], length)
    twiddle = single(np.repeat(turns, HALF, 3).transpose(1, 2, 0, 3).reshape(wav, padded, LANES))
    base_exact = cos_sin(wav * inner[:, None] * inner[None], length)
    base_exact = base_exact * ((inner[:, None] < rows) & (inner[None] < rows))
    base_exact = base_exact.reshape(2 * padded, padded).astype(np.float32)
    base_high = base_exact.astype(jnp.bfloat16)
    base_low = (base_exact - base_high.astype(np.float32)).astype(jnp.bfloat16)
    base = jnp.asarray(np.stack([base_high, base_low]))
    limits = truncation_limit.reshape(1, length)
    chunk_a = pltpu.VMEM((wav, rows, LANES), jnp.float32)
    chunk_b = pltpu.VMEM((wav, rows + group_rows, LANES), jnp.float32)
    everyone = wav * lev
    vmem, smem, anywhere = (pl.BlockSpec(memory_space=m) for m in (pltpu.VMEM, pltpu.SMEM, pl.ANY))
    f32, bf16 = jnp.float32, jnp.bfloat16
    filtered, energies, total = pl.pallas_call(
        functools.partial(fused_kernel, sizes),
        out_shape=(
            jax.ShapeDtypeStruct((slabs * rows, length), f32),
            jax.ShapeDtypeStruct((slabs,), f32),
            jax.ShapeDtypeStruct((1,), f32),
        ),
        in_specs=[vmem, vmem, smem, smem, smem, vmem, vmem] + [anywhere] * 4,
        out_specs=(vmem, smem, smem),
        scratch_shapes=[
            pltpu.VMEM((2, slabs * rows, length), bf16),
            pltpu.VMEM((2, length, 2 * LANES), bf16),
            pltpu.VMEM((quarters, 2, 3 * LANES, length), bf16),
            pltpu.VMEM(back_coarse.shape, f32),
            pltpu.VMEM(back_fine.shape, f32),
            pltpu.VMEM(twiddle.shape, f32),
            pltpu.VMEM(base.shape, bf16),
            chunk_a, chunk_a, chunk_b, chunk_b, chunk_a, chunk_a, chunk_b, chunk_b,
            pltpu.VMEM((wav, rows, LANES), f32),
            pltpu.VMEM((wav, padded, 2 * LANES), f32),
            pltpu.VMEM((wav, padded, 3 * LANES), f32),
            pltpu.VMEM((2, 8, LANES), f32),
            pltpu.VMEM((everyone, 2, 8, LANES), f32),
            pltpu.SemaphoreType.DMA((4,)),
            pltpu.SemaphoreType.DMA((4, wav)),
            pltpu.SemaphoreType.DMA((4, wav)),
            pltpu.SemaphoreType.DMA((everyone,)),
            pltpu.SemaphoreType.DMA((everyone,)),
            pltpu.SemaphoreType.DMA((5,)),
        ],
        compiler_params=pltpu.CompilerParams(
            collective_id=0, has_side_effects=True, vmem_limit_bytes=60 * 1024 * 1024
        ),
        name="fused_step",
    )(
        grid_field.reshape(slabs * rows, length), limits, diffusion_order, diffusion_strength, mass_weight,
        coarse, fine, back_coarse, back_fine, twiddle, base,
    )
    return filtered.reshape(slabs, rows, length), energies, total[0]


def fits(shape):
    slabs, rows, length = shape
    wav = lax.axis_size("wav")
    if wav != 8 or slabs != 2 or rows % 8 or length % 16 or length != rows * wav:
        return False
    columns = length * slabs // 2 // wav
    return length % 32 == 0 and LANES <= columns < LANES + LANES // 2


def local(grid_field, truncation_limit, diffusion_order, diffusion_strength, mass_weight):
    slab_count, row_count, length = grid_field.shape
    if fits(grid_field.shape):
        return fused(
            grid_field, truncation_limit, diffusion_order, diffusion_strength, mass_weight
        )
    cosine_table, sine_table = tables(length)
    filtered, partial_value = half_plane(
        grid_field, truncation_limit, diffusion_order, diffusion_strength, cosine_table, sine_table
    )
    total_slabs = lax.axis_size("lev") * slab_count
    energies = lax.psum(partial_value, "wav")
    weighted_sum = lax.psum(jnp.sum(mass_weight * energies), "lev")
    total_energy = weighted_sum / total_slabs
    return (filtered, energies, total_energy)


def solution(mesh):
    placed = (P("lev", "wav", None), P(), P("lev"), P("lev"), P("lev"))
    return jax.shard_map(
        local,
        mesh=mesh,
        in_specs=placed,
        out_specs=(P("lev", "wav", None), P("lev"), P()),
        check_vma=False,
    )
```

```python
import functools

import jax
import jax.numpy as jnp
import numpy as np
from jax import lax
from jax.experimental import pallas as pl
from jax.experimental.pallas import tpu as pltpu
from jax.sharding import PartitionSpec as P

product_precision = lax.Precision.HIGH


def tables(length):
    step = 32
    coarse = -(-length // step)
    columns = np.arange(length)
    high = 2.0 * np.pi / length * (np.arange(coarse)[:, None] * step * columns[None, :] % length)
    low = 2.0 * np.pi / length * (np.arange(step)[:, None] * columns[None, :] % length)
    cos_high, sin_high = (jnp.asarray(f(high), jnp.float32)[:, None] for f in (np.cos, np.sin))
    cos_low, sin_low = (jnp.asarray(f(low), jnp.float32)[None] for f in (np.cos, np.sin))
    cosine = cos_high * cos_low - sin_high * sin_low
    sine = sin_high * cos_low + cos_high * sin_low
    return tuple(t.reshape(coarse * step, length)[:length] for t in (cosine, sine))


def signed(positions, length):
    return jnp.where(positions < length // 2, positions, positions - length)


def transform(values, cosine_table, sine_table, direction):
    with_cosine = jnp.einsum("scpi,iq->scpq", values, cosine_table, precision=product_precision)
    with_sine = jnp.einsum("scpi,iq->scpq", values, sine_table, precision=product_precision)
    if direction < 0:
        real_part = with_cosine[:, 0] + with_sine[:, 1]
        imaginary = with_cosine[:, 1] - with_sine[:, 0]
    else:
        real_part = with_cosine[:, 0] - with_sine[:, 1]
        imaginary = with_cosine[:, 1] + with_sine[:, 0]
    return jnp.stack([real_part, imaginary], axis=1)


def damping(wave_rows, limits, length, diffusion_order, diffusion_strength):
    wave_first = signed(jnp.arange(length, dtype=jnp.int32), length)
    rows_float = wave_rows.astype(jnp.float32)
    first_float = wave_first.astype(jnp.float32)
    scaled_radius = (rows_float[:, None] ** 2 + first_float[None, :] ** 2) / (0.5 * length) ** 2
    inside = (jnp.abs(wave_first)[None, :] <= limits[:, None]).astype(jnp.float32)
    powered = jnp.power(scaled_radius[None], diffusion_order.astype(jnp.float32)[:, None, None])
    return inside[None] / (1.0 + diffusion_strength[:, None, None] * powered)


def mirrored(values):
    return jnp.roll(jnp.flip(values, -1), 1, -1)


def half_plane(
    grid_field, truncation_limit, diffusion_order, diffusion_strength, cosine_table, sine_table
):
    length = grid_field.shape[2]
    half = length // 2
    row_real = jnp.einsum("sij,jl->sli", grid_field, cosine_table[:, :half], precision=product_precision)
    row_imag = -jnp.einsum("sij,jl->sli", grid_field, sine_table[:, :half], precision=product_precision)
    nyquist = jnp.einsum("sij,j->si", grid_field, cosine_table[:, half], precision=product_precision)
    zero_row = (jnp.arange(half, dtype=jnp.int32) == 0)[None, :, None]
    row_imag = jnp.where(zero_row, nyquist[:, None, :], row_imag)
    along_rows = jnp.stack([row_real, row_imag], axis=1)
    spectrum = transform(
        lax.all_to_all(along_rows, "wav", split_axis=2, concat_axis=3, tiled=True),
        cosine_table,
        sine_table,
        -1,
    )
    column_count = spectrum.shape[2]
    wav_index = lax.axis_index("wav")
    offset = wav_index * column_count
    wave_rows = offset + jnp.arange(column_count, dtype=jnp.int32)
    limits = lax.dynamic_slice(truncation_limit, (offset,), (column_count,))
    damp_main = damping(wave_rows, limits, length, diffusion_order, diffusion_strength)
    nyquist_rows = signed(jnp.full((1,), half, jnp.int32), length)
    damp_top = damping(
        nyquist_rows, truncation_limit[half : half + 1], length, diffusion_order, diffusion_strength
    )[:, 0]
    damped = spectrum * damp_main[:, None]
    packed_real = spectrum[:, 0, 0, :]
    packed_imag = spectrum[:, 1, 0, :]
    back_real = mirrored(packed_real)
    back_imag = mirrored(packed_imag)
    zero_real = (packed_real + back_real) * 0.5 * damp_main[:, 0]
    zero_imag = (packed_imag - back_imag) * 0.5 * damp_main[:, 0]
    top_real = (packed_imag + back_imag) * 0.5 * damp_top
    top_imag = (back_real - packed_real) * 0.5 * damp_top
    is_zero = wave_rows == 0
    column_weight = jnp.where(is_zero, 0.0, 2.0).astype(jnp.float32)
    edge = jnp.sum(zero_real**2 + zero_imag**2 + top_real**2 + top_imag**2, axis=-1)
    main_sum = jnp.sum(damped * damped * column_weight[None, None, :, None], axis=(1, 2, 3))
    partial_value = (main_sum + jnp.where(wav_index == 0, edge, 0.0)) / float(length) ** 4
    zero_column = is_zero[None, :, None]
    repacked = jnp.stack(
        [
            jnp.where(zero_column, (zero_real - top_imag)[:, None, :], damped[:, 0]),
            jnp.where(zero_column, (zero_imag + top_real)[:, None, :], damped[:, 1]),
        ],
        axis=1,
    )
    along_first = transform(repacked, cosine_table, sine_table, 1)
    inverse_area = 1.0 / float(length) ** 2
    received = lax.all_to_all(along_first, "wav", split_axis=3, concat_axis=2, tiled=True)
    row_weight = jnp.where(jnp.arange(half, dtype=jnp.int32) == 0, 1.0, 2.0).astype(jnp.float32)[
        :, None
    ]
    with_cosine = jnp.einsum(
        "spi,pj->sij", received[:, 0] * row_weight, cosine_table[:half], precision=product_precision
    )
    with_sine = jnp.einsum(
        "spi,pj->sij", received[:, 1] * row_weight, sine_table[:half], precision=product_precision
    )
    top_term = received[:, 1, 0, :][:, :, None] * cosine_table[half][None, None, :]
    filtered = (with_cosine - with_sine + top_term) * inverse_area
    return (filtered, partial_value)


LANES = 128
HALF = LANES // 2
MESH = pl.DeviceIdType.MESH


def halves(values):
    high = values.astype(jnp.bfloat16)
    return high, (values - high.astype(jnp.float32)).astype(jnp.bfloat16)


def product(left, right):
    dot = functools.partial(jnp.dot, preferred_element_type=jnp.float32)
    return dot(left[0], right[0]) + dot(left[1], right[0]) + dot(left[0], right[1])


def swap(value):
    count = value.shape[1] // LANES
    turned = [pltpu.roll(value[:, n * LANES : (n + 1) * LANES], HALF, 1) for n in range(count)]
    return jnp.concatenate(turned, 1) if count > 1 else turned[0]


def eight_points(x, sign, signs):
    turn = signs if sign < 0 else -signs

    def four(p, q, r, t):
        a0, a1, a2, a3 = p + r, p - r, q + t, swap(q - t) * turn
        return a0 + a2, a1 + a3, a0 - a2, a1 - a3

    e = four(x[0], x[2], x[4], x[6])
    o = four(x[1], x[3], x[5], x[7])
    root = 0.5**0.5
    odd = (
        o[0],
        root * (o[1] + swap(o[1]) * turn),
        swap(o[2]) * turn,
        root * (swap(o[3]) * turn - o[3]),
    )
    return [e[n] + odd[n] for n in range(4)] + [e[n] - odd[n] for n in range(4)]


def pieces(rows, group_rows, groups):
    found = []
    for group in range(groups):
        start, stop = group * group_rows, min((group + 1) * group_rows, 2 * rows)
        while start < stop:
            part = start // rows
            end = min(stop, (part + 1) * rows)
            found.append((group, start - group * group_rows, part, start - part * rows, end - start))
            start = end
    return found


def fused_kernel(
    sizes,
    grid_ref, limit_ref, order_ref, strength_ref, mass_ref, coarse_ref, fine_ref,
    back_coarse_hbm, back_fine_hbm, twiddle_hbm, base_hbm,
    out_ref, energy_ref, total_ref,
    grid_parts, table, back_table, back_coarse, back_fine, twiddle, base,
    sent_a, got_a, sent_b, got_b, back_a, home_a, back_b, home_b,
    rest, work, damp, energy_mine, energy_all,
    load_sems, send_sems, recv_sems, e_send_sems, e_recv_sems, local_sems,
):
    slabs, rows, length, wav, lev, quarters, columns, padded, tail, groups, group_rows, fine_rows = sizes
    everyone = lev * wav
    half = length // 2
    me = lax.axis_index("wav")
    level = lax.axis_index("lev")
    my_quarter, my_slab = me // slabs, me % slabs
    flat = level * wav + me

    barrier = pltpu.get_barrier_semaphore()

    @pl.loop(1, everyone)
    def _(step):
        target = (flat + step) % everyone
        pl.semaphore_signal(barrier, inc=1, device_id=(target // wav, target % wav), device_id_type=MESH)

    loads = [
        pltpu.make_async_copy(src, dst, load_sems.at[n])
        for n, (src, dst) in enumerate(
            ((twiddle_hbm, twiddle), (base_hbm, base), (back_coarse_hbm, back_coarse), (back_fine_hbm, back_fine))
        )
    ]
    for load in loads:
        load.start()
    high, low = halves(grid_ref[...])
    grid_parts[0] = high
    grid_parts[1] = low

    def quarter_of(step):
        down, across = 1 - step % 2, 1 - step // 2
        y, x = my_quarter // 2, my_quarter % 2
        return (y + down - 2 * y * down) * 2 + (x + across - 2 * x * across)

    def push(source, target, phase, w):
        @pl.when(w != me)
        def _():
            pltpu.make_async_remote_copy(
                src_ref=source.at[w], dst_ref=target.at[me],
                send_sem=send_sems.at[phase, w], recv_sem=recv_sems.at[phase, me],
                device_id=(level, w), device_id_type=MESH,
            ).start()

        @pl.when(w == me)
        def _():
            pltpu.make_async_copy(source.at[w], target.at[w], local_sems.at[phase]).start()

    def arrive(source, target, phase, w):
        @pl.when(w != me)
        def _():
            pltpu.make_async_remote_copy(
                src_ref=source.at[w], dst_ref=target.at[w],
                send_sem=send_sems.at[phase, w], recv_sem=recv_sems.at[phase, w],
                device_id=(level, w), device_id_type=MESH,
            ).wait()

        @pl.when(w == me)
        def _():
            pltpu.make_async_copy(source.at[w], target.at[w], local_sems.at[phase]).wait()

    lane = lax.broadcasted_iota(jnp.int32, (1, LANES), 1)
    signs = jnp.where(lane < HALF, 1.0, -1.0)
    in_part = [(lane >= part * HALF) & (lane < part * HALF + tail) for part in range(2)]
    layout = pieces(rows, group_rows, groups)

    def pack(tile):
        shifted = {}
        for group, at, part, start, count in layout:
            piece = jnp.where(in_part[part], tile(start, count), 0.0)
            shift = (group * tail - part * HALF) % LANES
            shifted.setdefault(group, []).append(pltpu.roll(piece, shift, 1) if shift else piece)
        packed = jnp.zeros((group_rows, LANES), jnp.float32)
        for found in shifted.values():
            whole = jnp.concatenate(found, 0) if len(found) > 1 else found[0]
            if whole.shape[0] < group_rows:
                fill = jnp.zeros((group_rows - whole.shape[0], LANES), jnp.float32)
                whole = jnp.concatenate([whole, fill], 0)
            packed = packed + whole
        return packed

    def unpack(packed):
        found = {0: [], 1: []}
        for group, at, part, start, count in layout:
            piece = packed[at : at + count]
            shift = (part * HALF - group * tail) % LANES
            piece = pltpu.roll(piece, shift, 1) if shift else piece
            found[part].append(jnp.where(in_part[part], piece, 0.0))
        return jnp.concatenate(found[0], 0) + jnp.concatenate(found[1], 0)

    def forward(first, count, phase, source, target):
        @pl.loop(0, quarters)
        def _(step):
            quarter = quarter_of(step)
            columns_of = slice(first * LANES, (first + count) * LANES)
            cos_f, sin_f = fine_ref[0, quarter, :, columns_of], fine_ref[1, quarter, :, columns_of]

            @pl.loop(0, length // fine_rows, unroll=2)
            def _(block):
                cos_c = coarse_ref[0, quarter, pl.ds(block, 1)][:, columns_of]
                sin_c = coarse_ref[1, quarter, pl.ds(block, 1)][:, columns_of]
                span = pl.ds(pl.multiple_of(block * fine_rows, fine_rows), fine_rows)
                value_high, value_low = halves(cos_c * cos_f - sin_c * sin_f)
                table[0, span, : count * LANES] = value_high
                table[1, span, : count * LANES] = value_low

            result = product(
                (grid_parts[0], grid_parts[1]), (table[0, :, : count * LANES], table[1, :, : count * LANES])
            )
            for slab in range(slabs):
                w = quarter * slabs + slab
                source[w, :rows] = result[slab * rows : (slab + 1) * rows, :LANES]
                if count > 1:
                    source[w, rows:] = pack(
                        lambda start, many: result[slab * rows + start : slab * rows + start + many, LANES:]
                    )

            if first == 0:
                @pl.when(step == 0)
                def _():
                    pl.semaphore_wait(barrier, everyone - 1)

            for slab in range(slabs):
                push(source, target, phase, quarter * slabs + slab)

    forward(0, 1, 0, sent_a, got_a)
    forward(1, 2, 1, sent_b, got_b)

    loads[0].wait()
    loads[1].wait()
    place = lax.broadcasted_iota(jnp.int32, (1, 3 * LANES), 1)
    column = place // LANES * HALF + place % HALF
    wave = my_quarter * columns + column
    valid = (column < columns) | ((column == columns) & (wave == half))
    single = (wave == 0) | (wave == half)
    out_weight = jnp.where(single, 1.0, 2.0) / float(length) ** 2
    energy_weight = jnp.where(single, 1.0, 0.5)
    all_limits = limit_ref[...]
    limits = jnp.full((1, 3 * LANES), -1, jnp.int32)
    for quarter in range(quarters):
        found = []
        for tile in range(3):
            start = quarter * columns + tile * HALF
            found += [all_limits[:, start : start + HALF]] * 2
        limits = jnp.where(my_quarter == quarter, jnp.concatenate(found, 1), limits)
    limits = jnp.where(valid, limits, -1)
    order = order_ref[my_slab]
    strength = strength_ref[my_slab]
    wave_square = wave.astype(jnp.float32) ** 2

    @pl.loop(0, wav)
    def _(m):
        row = lax.broadcasted_iota(jnp.int32, (padded, 1), 0)
        q = row * wav + m
        signed_q = jnp.where(q < half, q, q - length)
        radius = (wave_square + signed_q.astype(jnp.float32) ** 2) / (0.5 * length) ** 2
        square = radius * radius
        powered = jnp.where(order >= 3, square, 1.0) * jnp.where(order % 2 == 1, radius, square)
        inside = (jnp.abs(signed_q) <= limits) & (row < rows)
        damp[m] = jnp.where(inside, out_weight / (1.0 + strength * powered), 0.0)
        work[m, rows:] = jnp.zeros((padded - rows, 2 * LANES), jnp.float32)

    def along(value):
        value_high, value_low = halves(value)
        stacked = jnp.concatenate([value_high, value_high, value_low], 0)
        return jnp.dot(base[...], stacked, preferred_element_type=jnp.float32)

    block_rows = 24

    def in_blocks(body):
        @pl.loop(0, rows // block_rows)
        def _(block):
            body(pl.multiple_of(block * block_rows, 8), block_rows)

        if rows % block_rows:
            body(rows - rows % block_rows, rows % block_rows)

    def middle(first, count, phase, got, back, home, announce):
        spans = slice(0, count * LANES)
        all_signs = jnp.concatenate([signs] * count, 1)

        def split(start, many):
            span = pl.ds(start, many)
            for tile in range(count):
                x = [rest[w, span] if tile else got[w, span] for w in range(wav)]
                for m, value in enumerate(eight_points(x, -1, signs)):
                    work[m, span, tile * LANES : (tile + 1) * LANES] = value

        in_blocks(split)

        def one_residue(m, sums):
            packed_turn = twiddle[m]
            other_turn = swap(packed_turn)
            cos_t = jnp.concatenate([jnp.where(lane < HALF, packed_turn, other_turn)] * count, 1)
            sin_t = jnp.concatenate([jnp.where(lane < HALF, other_turn, -packed_turn)] * count, 1)
            value = work[m, :, spans]
            both = along(value * cos_t + swap(value) * sin_t)
            value = both[:padded] + swap(both[padded:]) * all_signs
            value = value * damp[m, :, first * LANES : (first + count) * LANES]
            sums = sums + jnp.sum((value * value).reshape(padded // 8, 8, count * LANES), axis=0)
            both = along(value)
            value = both[:padded] - swap(both[padded:]) * all_signs
            work[m, :, spans] = value * cos_t - swap(value) * sin_t
            return sums

        sums = jnp.zeros((8, count * LANES), jnp.float32)
        for m in range(wav):
            sums = one_residue(m, sums)
        sums = sums * energy_weight[:, first * LANES : (first + count) * LANES]

        announce(sum(sums[:, n * LANES : (n + 1) * LANES] for n in range(count)))

        def join(start, many):
            span = pl.ds(start, many)
            for tile in range(count):
                v = [work[m, span, tile * LANES : (tile + 1) * LANES] for m in range(wav)]
                for w, value in enumerate(eight_points(v, 1, signs)):
                    if tile:
                        rest[w, span] = value
                    else:
                        back[w, span] = value

        in_blocks(join)

        @pl.loop(0, quarters)
        def _(step):
            for slab in range(slabs):
                w = quarter_of(step) * slabs + slab
                if count > 1:
                    back[w, rows:] = pack(lambda start, many: rest[w, start : start + many])
                push(back, home, phase, w)

    @pl.loop(0, wav)
    def _(w):
        arrive(sent_a, got_a, 0, w)

    def energy_copy(target_flat, slot):
        return pltpu.make_async_remote_copy(
            src_ref=energy_mine, dst_ref=energy_all.at[slot],
            send_sem=e_send_sems.at[target_flat], recv_sem=e_recv_sems.at[slot],
            device_id=(target_flat // wav, target_flat % wav), device_id_type=MESH,
        )

    def announce_first(sums):
        energy_mine[0] = sums

    def announce_last(sums):
        sums = sums + energy_mine[0]
        energy_mine[0] = sums
        energy_mine[1] = sums * mass_ref[my_slab]

        @pl.loop(1, everyone)
        def _(step):
            energy_copy((flat + step) % everyone, flat).start()

        pltpu.make_async_copy(energy_mine, energy_all.at[flat], local_sems.at[4]).start()

    middle(0, 1, 2, got_a, back_a, home_a, announce_first)

    loads[2].wait()
    loads[3].wait()
    blocks = 3 * LANES // fine_rows

    @pl.loop(0, quarters)
    def _(quarter):
        @pl.loop(0, blocks)
        def _(block):
            at = quarter * blocks + block
            cos_c, sin_c = back_coarse[0, pl.ds(at, 1)], back_coarse[1, pl.ds(at, 1)]
            span = pl.ds(pl.multiple_of(block * fine_rows, fine_rows), fine_rows)
            value_high, value_low = halves(cos_c * back_fine[0] - sin_c * back_fine[1])
            back_table[quarter, 0, span] = value_high
            back_table[quarter, 1, span] = value_low

    out_ref[...] = jnp.zeros_like(out_ref)

    @pl.loop(0, wav)
    def _(w):
        arrive(sent_b, got_b, 1, w)
        rest[w] = unpack(got_b[w, rows:])

    middle(1, 2, 3, got_b, back_b, home_b, announce_last)
    own_energy = pltpu.make_async_copy(energy_mine, energy_all.at[flat], local_sems.at[4])

    def finish(first, count, phase, back, home):
        @pl.loop(0, quarters)
        def _(step):
            quarter = quarter_of((step + quarters - 1) % quarters)
            stacked = []
            for slab in range(slabs):
                w = quarter * slabs + slab
                arrive(back, home, phase, w)
                tiles = [home[w, :rows]]
                if count > 1:
                    tiles.append(unpack(home[w, rows:]))
                stacked.append(jnp.concatenate(tiles, 1) if count > 1 else tiles[0])
            left = halves(jnp.concatenate(stacked, 0))
            span = slice(first * LANES, (first + count) * LANES)
            out_ref[...] += product(left, (back_table[quarter, 0, span], back_table[quarter, 1, span]))

    finish(0, 1, 2, back_a, home_a)
    finish(1, 2, 3, back_b, home_b)
    own_energy.wait()

    @pl.loop(1, everyone)
    def _(step):
        source = (flat + step) % everyone
        energy_copy(source, source).wait()

    total = energy_all[0, 1]
    for n in range(1, everyone):
        total = total + energy_all[n, 1]
    total_ref[0] = jnp.sum(total) / (lev * slabs)
    for slab in range(slabs):
        tile = energy_all[level * wav + slab, 0]
        for quarter in range(1, quarters):
            tile = tile + energy_all[level * wav + quarter * slabs + slab, 0]
        energy_ref[slab] = jnp.sum(tile)


def cos_sin(phases, length):
    angles = 2.0 * np.pi / length * (phases % length)
    return np.stack([np.cos(angles), np.sin(angles)])


def fused(grid_field, truncation_limit, diffusion_order, diffusion_strength, mass_weight):
    slabs, rows, length = grid_field.shape
    wav, lev = lax.axis_size("wav"), lax.axis_size("lev")
    quarters = wav // slabs
    columns = length // 2 // quarters
    tail = columns + 1 - LANES
    groups = LANES // tail
    group_rows = -(-(-(-2 * rows // groups)) // 8) * 8
    padded = -(-rows // 16) * 16
    fine_rows = 32
    sizes = (slabs, rows, length, wav, lev, quarters, columns, padded, tail, groups, group_rows, fine_rows)
    starts = np.arange(quarters) * columns
    place = np.arange(3 * LANES)
    column = place // LANES * HALF + place % HALF
    phase = (place % LANES >= HALF) * (length // 4)
    waves = starts[:, None] + column[None]
    steps = np.arange(length // fine_rows) * fine_rows
    near = np.arange(fine_rows)
    positions = np.arange(length)
    single = lambda array: jnp.asarray(array, jnp.float32)
    coarse = single(cos_sin(steps[None, :, None] * waves[:, None, :], length))
    fine = single(cos_sin(near[None, :, None] * waves[:, None, :] + phase, length))
    back_starts = waves[:, ::fine_rows].reshape(-1)
    back_phase = np.tile(phase[::fine_rows], quarters)
    back_coarse = single(cos_sin(back_starts[:, None] * positions[None] + back_phase[:, None], length))
    back_fine = single(cos_sin(near[:, None] * positions[None], length))
    inner = np.arange(padded)
    turns = cos_sin(np.arange(wav)[:, None, None] * inner[None, :, None], length)
    twiddle = single(np.repeat(turns, HALF, 3).transpose(1, 2, 0, 3).reshape(wav, padded, LANES))
    base_exact = cos_sin(wav * inner[:, None] * inner[None], length)
    base_exact = base_exact * ((inner[:, None] < rows) & (inner[None] < rows))
    base_exact = base_exact.reshape(2 * padded, padded).astype(np.float32)
    base_high = base_exact.astype(jnp.bfloat16)
    base_low = (base_exact - base_high.astype(np.float32)).astype(jnp.bfloat16)
    base = jnp.asarray(np.concatenate([base_high, base_low, base_high], 1))
    limits = truncation_limit.reshape(1, length)
    chunk_a = pltpu.VMEM((wav, rows, LANES), jnp.float32)
    chunk_b = pltpu.VMEM((wav, rows + group_rows, LANES), jnp.float32)
    everyone = wav * lev
    vmem, smem, anywhere = (pl.BlockSpec(memory_space=m) for m in (pltpu.VMEM, pltpu.SMEM, pl.ANY))
    f32, bf16 = jnp.float32, jnp.bfloat16
    filtered, energies, total = pl.pallas_call(
        functools.partial(fused_kernel, sizes),
        out_shape=(
            jax.ShapeDtypeStruct((slabs * rows, length), f32),
            jax.ShapeDtypeStruct((slabs,), f32),
            jax.ShapeDtypeStruct((1,), f32),
        ),
        in_specs=[vmem, vmem, smem, smem, smem, vmem, vmem] + [anywhere] * 4,
        out_specs=(vmem, smem, smem),
        scratch_shapes=[
            pltpu.VMEM((2, slabs * rows, length), bf16),
            pltpu.VMEM((2, length, 2 * LANES), bf16),
            pltpu.VMEM((quarters, 2, 3 * LANES, length), bf16),
            pltpu.VMEM(back_coarse.shape, f32),
            pltpu.VMEM(back_fine.shape, f32),
            pltpu.VMEM(twiddle.shape, f32),
            pltpu.VMEM(base.shape, bf16),
            chunk_a, chunk_a, chunk_b, chunk_b, chunk_a, chunk_a, chunk_b, chunk_b,
            pltpu.VMEM((wav, rows, LANES), f32),
            pltpu.VMEM((wav, padded, 2 * LANES), f32),
            pltpu.VMEM((wav, padded, 3 * LANES), f32),
            pltpu.VMEM((2, 8, LANES), f32),
            pltpu.VMEM((everyone, 2, 8, LANES), f32),
            pltpu.SemaphoreType.DMA((4,)),
            pltpu.SemaphoreType.DMA((4, wav)),
            pltpu.SemaphoreType.DMA((4, wav)),
            pltpu.SemaphoreType.DMA((everyone,)),
            pltpu.SemaphoreType.DMA((everyone,)),
            pltpu.SemaphoreType.DMA((5,)),
        ],
        compiler_params=pltpu.CompilerParams(
            collective_id=0, has_side_effects=True, vmem_limit_bytes=60 * 1024 * 1024
        ),
        name="fused_step",
    )(
        grid_field.reshape(slabs * rows, length), limits, diffusion_order, diffusion_strength, mass_weight,
        coarse, fine, back_coarse, back_fine, twiddle, base,
    )
    return filtered.reshape(slabs, rows, length), energies, total[0]


def fits(shape):
    slabs, rows, length = shape
    wav = lax.axis_size("wav")
    if wav != 8 or slabs != 2 or rows % 8 or length % 16 or length != rows * wav:
        return False
    columns = length * slabs // 2 // wav
    return length % 32 == 0 and LANES <= columns < LANES + LANES // 2


def local(grid_field, truncation_limit, diffusion_order, diffusion_strength, mass_weight):
    slab_count, row_count, length = grid_field.shape
    if fits(grid_field.shape):
        return fused(
            grid_field, truncation_limit, diffusion_order, diffusion_strength, mass_weight
        )
    cosine_table, sine_table = tables(length)
    filtered, partial_value = half_plane(
        grid_field, truncation_limit, diffusion_order, diffusion_strength, cosine_table, sine_table
    )
    total_slabs = lax.axis_size("lev") * slab_count
    energies = lax.psum(partial_value, "wav")
    weighted_sum = lax.psum(jnp.sum(mass_weight * energies), "lev")
    total_energy = weighted_sum / total_slabs
    return (filtered, energies, total_energy)


def solution(mesh):
    placed = (P("lev", "wav", None), P(), P("lev"), P("lev"), P("lev"))
    return jax.shard_map(
        local,
        mesh=mesh,
        in_specs=placed,
        out_specs=(P("lev", "wav", None), P("lev"), P()),
        check_vma=False,
    )
```
